256 devices in a mesh: section: 4 (over y), row: 8 (over x, core), col: 8 (over z).
Axes of the slice: x: 4, y: 4, z: 8, core: 2. Of those that a mesh axis runs over, the one named last changes fastest.
Arguments:
- cotangent: float32 [4, 128, 4096], P('section', None, ('row', 'col')), may hold values from -6 to 6
- incoming: float32 [4, 128, 4096], P('section', None, ('row', 'col')), may hold values from -6 to 6
- upd_u: float32 [4, 8, 128, 4096], P('section', None, None, ('row', 'col')), may hold values from -4 to 4
- upd_v: float32 [4, 8, 128, 4096], P('section', None, None, ('row', 'col')), may hold values from -0.0078125 to 0.0078125
- saved_x: bfloat16 [4, 4, 128, 4096], P('section', None, None, ('row', 'col')), may hold values from -6 to 6
- saved_h: bfloat16 [4, 4, 2, 128, 14336], P('section', None, None, None, 'col'), may hold values from -6 to 6
- norm_gain: float32 [4, 4096], P('section', ('row', 'col')), may hold values from 0.25 to 1.75
- w_gate: bfloat16 [4, 4096, 14336], P('section', 'row', 'col'), may hold values from -0.09375 to 0.09375
- w_up: bfloat16 [4, 4096, 14336], P('section', 'row', 'col'), may hold values from -0.09375 to 0.09375
- w_down: bfloat16 [4, 14336, 4096], P('section', 'col', 'row'), may hold values from -0.046875 to 0.046875
Outputs:
- new_cotangent: float32 [4, 128, 4096], P('section', None, ('row', 'col'))
- residual_out: float32 [4, 128, 4096], P('section', None, ('row', 'col'))
The draws below stay inside these ranges and needn't reach their ends.
All inputs are finite; a program needn't handle non-finite values.
Results may differ from the reference program's by a relative error of at most 0.014.
Values may be sent and summed in bfloat16 or wider, within the bound.
A program may use at most 64 MiB of HBM per device.

```python
import jax
import jax.numpy as jnp
from jax import lax

D = 4096
FF = 14336
ROWS = 128
UPD = 8
LAYERS = 4
MB = 4


def shard_levels(stream_key, shape, cuts, least, top_value):
    def one(axis_at, blocks):
        draws = jax.random.uniform(jax.random.fold_in(jax.random.fold_in(stream_key, 6), axis_at), (blocks,), jnp.float32, least / len(cuts), top_value / len(cuts))
        return jnp.repeat(jnp.exp(draws), shape[axis_at] // blocks).reshape((-1,) + (1,) * (len(shape) - axis_at - 1))

    level = one(*cuts[0])
    for cut in cuts[1:]:
        level = level * one(*cut)
    return level


def noise(rng, extent, deviation, reach, split=(), kind=jnp.bfloat16):
    array = jax.random.normal(rng, extent, jnp.float32) * deviation
    if len(split) > 0:
        array = shard_levels(rng, extent, split, -0.22, 0.18) * array
    return jnp.clip(array, min=-reach, max=reach).astype(kind)


def setup_inputs(seed: int = 0) -> dict:
    streams_of = jax.random.split(jax.random.key(seed), 11)
    return {
        "cotangent": noise(streams_of[0], (MB, ROWS, D), 1.0, 6.0, ((0, 4), (2, 64)), jnp.float32),
        "incoming": noise(streams_of[1], (MB, ROWS, D), 1.0, 6.0, ((0, 4), (2, 64)), jnp.float32),
        "upd_u": noise(streams_of[2], (MB, UPD, ROWS, D), 0.3, 4.0, ((0, 4), (3, 64)), jnp.float32),
        "upd_v": noise(streams_of[3], (MB, UPD, ROWS, D), (ROWS * D) ** -0.5, 0.0078125, ((0, 4), (3, 64)), jnp.float32),
        "saved_x": noise(streams_of[4], (LAYERS, MB, ROWS, D), 1.0, 6.0, ((0, 4), (3, 64))),
        "saved_h": noise(streams_of[5], (LAYERS, MB, 2, ROWS, FF), 1.5, 6.0, ((0, 4), (4, 8))),
        "norm_gain": jnp.clip(1.0 + 0.15 * jax.random.normal(streams_of[6], (LAYERS, D), jnp.float32), 0.25, 1.75),
        "w_gate": noise(streams_of[7], (LAYERS, D, FF), D ** -0.5, 0.09375, ((0, 4), (1, 8), (2, 8))),
        "w_up": noise(streams_of[8], (LAYERS, D, FF), D ** -0.5, 0.09375, ((0, 4), (1, 8), (2, 8))),
        "w_down": noise(streams_of[9], (LAYERS, FF, D), FF ** -0.5, 0.046875, ((0, 4), (1, 8), (2, 8))),
    }


eps = 1e-05

def layer_back(c, x, hpair, gain, wg, wu, wd):
    gy = c.astype(jnp.bfloat16)
    ga = jnp.dot(gy, wd.T, preferred_element_type=jnp.float32)
    hg = hpair[0].astype(jnp.float32)
    hu = hpair[1].astype(jnp.float32)
    sig = jax.nn.sigmoid(hg)
    grad_gate = (ga * hu * sig * (1.0 + hg * (1.0 - sig))).astype(jnp.bfloat16)
    grad_up = (ga * hg * sig).astype(jnp.bfloat16)
    normgrad = jnp.dot(grad_gate, wg.T, preferred_element_type=jnp.float32) + jnp.dot(grad_up, wu.T, preferred_element_type=jnp.float32)
    xf = x.astype(jnp.float32)
    rstd = lax.rsqrt(lax.optimization_barrier(jnp.sum(xf * xf, axis=-1, keepdims=True)) / D + eps)
    scaled = gain * normgrad
    inner = lax.optimization_barrier(jnp.sum(scaled * xf, axis=-1, keepdims=True)) / D
    return c + rstd * scaled - xf * (rstd * rstd * rstd) * inner

def reference(cotangent, incoming, upd_u, upd_v, saved_x, saved_h, norm_gain, w_gate, w_up, w_down):
    new_list = []
    res_list = []
    for micro in range(MB):
        carry = cotangent[micro]
        for layer in range(LAYERS - 1, -1, -1):
            carry = layer_back(carry, saved_x[layer, micro], saved_h[layer, micro], norm_gain[layer], w_gate[layer], w_up[layer], w_down[layer])
        resid = carry + incoming[micro] - cotangent[micro]
        dots = jnp.einsum('urd,rd->u', upd_v[micro], resid, precision=lax.Precision.HIGHEST)
        update = jnp.einsum('u,urd->rd', dots, upd_u[micro], precision=lax.Precision.HIGHEST)
        new_list.append(cotangent[micro] + resid - update)
        res_list.append(resid)
    return (jnp.stack(new_list), jnp.stack(res_list))
```

```python
import jax
import jax.numpy as jnp
from jax import lax
from jax.experimental import pallas as pl
from jax.experimental.pallas import tpu as pltpu
from jax.sharding import PartitionSpec as P

D = 4096
FF = 14336
ROWS = 128
UPD = 8
MB = 4
SECTIONS, ROW, COL = 4, 8, 8
XS = ROW // 2
CHUNK = D // (ROW * COL)
FEATS = D // ROW
HID = FF // COL
HALF = HID // 2
PIECE = HID // ROW
FAR_Z = (4, 3, 5, 2, 6, 1, 7)
FAR_X = (2, 1, 3)
SLOTS = MB + 3

eps = 1e-05
bf16 = jnp.bfloat16
f32 = jnp.float32
MESH = pl.DeviceIdType.MESH


def kernel(
    cot_h, inc_h, u_h, v_h, x_h, h_h, gain_h, wg_h, wu_h, wd_h,
    new_o, res_o,
    cot_v, inc_v, u_v, v_v, x_v, h_v, gain_v, wg_v, wu_v, wd_v,
    cot_t, inc_t, u_t, v_t, x_t, gain_t, gx, slope,
    start, gy, gys, carry, after, d1s, d1r, own, xsd, xrv, mine, ga, grads, acc, zs, zr,
    ixs, ixr, izs, izr, sqs, sqz, sqm, sqx, rstd, home, dxs, dxr, dzs, dzr,
    load, first, ss, rs, one_s, one_r,
):
    s = lax.axis_index("section")
    r = lax.axis_index("row")
    c = lax.axis_index("col")
    core = lax.rem(r, 2)
    x = lax.div(r, 2)
    mate = r + 1 - 2 * core

    def at_col(k):
        return lax.rem(c + k, COL)

    def at_x(k):
        return lax.rem(x + k, XS)

    def remote(src, dst, send, recv, device):
        return pltpu.make_async_remote_copy(
            src_ref=src, dst_ref=dst, send_sem=send, recv_sem=recv, device_id=device, device_id_type=MESH
        )

    def arrived(ref, recv):
        remote(ref, ref, one_s.at[0], recv, (s, mate, c)).wait_recv()

    def left(ref, send):
        remote(ref, ref, send, one_r.at[0], (s, mate, c)).wait_send()

    loads = {}
    for i, (name, src, dst) in enumerate(
        (
            ("cot", cot_h.at[0], cot_v),
            ("gain", gain_h, gain_v),
            ("x", x_h.at[0], x_v),
            ("wd", wd_h.at[0], wd_v),
            ("h", h_h.at[0], h_v),
            ("wg0", wg_h.at[0, :, pl.ds(0, HALF)], wg_v.at[0]),
            ("wg1", wg_h.at[0, :, pl.ds(HALF, HALF)], wg_v.at[1]),
            ("wu0", wu_h.at[0, :, pl.ds(0, HALF)], wu_v.at[0]),
            ("wu1", wu_h.at[0, :, pl.ds(HALF, HALF)], wu_v.at[1]),
            ("inc", inc_h.at[0], inc_v),
            ("u", u_h.at[0], u_v),
            ("v", v_h.at[0], v_v),
        )
    ):
        loads[name] = pltpu.make_async_copy(src, dst, load.at[i])
        loads[name].start()

    barrier = pltpu.get_barrier_semaphore()
    for ds in range(SECTIONS):
        for dc in range(COL):
            if ds or dc:
                there = (lax.rem(s + ds, SECTIONS), r, at_col(dc))
                pl.semaphore_signal(barrier, inc=1, device_id=there, device_id_type=MESH)
    for dr in range(1, ROW):
        pl.semaphore_signal(barrier, inc=1, device_id=(s, lax.rem(r + dr, ROW), c), device_id_type=MESH)

    loads["cot"].wait()
    cot_t[...] = cot_v[...].T
    start[...] = cot_t[...].astype(bf16)
    pl.semaphore_wait(barrier, SECTIONS * COL - 1 + ROW - 1)

    LAST = SECTIONS - 1
    mb_home = s

    @pl.when(s == LAST)
    def _():
        gy[LAST, c] = start[...]
        carry[LAST] = cot_t[...]
        for k in FAR_Z:
            remote(start, gy.at[LAST, c], first.at[0], rs.at[0, LAST], (LAST, r, at_col(k))).start()

    @pl.when(s != LAST)
    def _():
        for k in (*FAR_Z, 0):
            remote(start, gy.at[mb_home, c], first.at[0], rs.at[0, mb_home], (LAST, r, at_col(k))).start()
        remote(cot_t, carry.at[mb_home], first.at[1], rs.at[1, mb_home], (LAST, r, c)).start()

    loads["gain"].wait()
    loads["x"].wait()
    gain_t[...] = jnp.broadcast_to(gain_v[...], (ROWS, CHUNK)).T
    sums = []
    for m in range(MB):
        xt = x_v[m].astype(f32).T
        x_t[m] = xt
        gx[c, m] = (gain_t[...] * xt).astype(bf16)
        sums.append(jnp.sum(xt * xt, axis=0, keepdims=True))
    sums = jnp.concatenate(sums + sums, axis=0)
    sqs[...] = sums
    sqz[c] = sums
    for k in FAR_Z:
        remote(gx.at[c], gx.at[c], one_s.at[1], one_r.at[1], (s, r, at_col(k))).start()
        remote(sqs, sqz.at[c], one_s.at[2], one_r.at[2], (s, r, at_col(k))).start()

    def slopes(m):
        for half in range(2):
            for b in range(7):
                at = pl.ds(half * HALF + b * 128, 128)
                hg = h_v[m, 0, :, at].astype(f32)
                hu = h_v[m, 1, :, at].astype(f32)
                sig = jax.nn.sigmoid(hg)
                slope[m, 0, half, pl.ds(b * 128, 128)] = (hu * sig * (1.0 + hg * (1.0 - sig))).T
                slope[m, 1, half, pl.ds(b * 128, 128)] = (hg * sig).T

    def epilogue_inputs():
        inc_t[...] = inc_v[...].T
        for i in range(UPD):
            u_t[i] = u_v[i].T
            v_t[i] = v_v[i].T

    loads["h"].wait()
    loads["inc"].wait()
    loads["u"].wait()
    loads["v"].wait()

    @pl.when(s != LAST)
    def _():
        epilogue_inputs()

        def body(m, carry_):
            slopes(m)
            return carry_

        lax.fori_loop(0, MB, body, 0)

    @pl.when(s == LAST)
    def _():
        slopes(LAST)

    for name in ("wd", "wg0", "wg1", "wu0", "wu1"):
        loads[name].wait()

    def hidden(m):
        @pl.when(jnp.logical_and(s == LAST, m == LAST))
        def _():
            arrived(gy.at[m, pl.ds(0, COL - 1)], rs.at[0, m])

        @pl.when(jnp.logical_not(jnp.logical_and(s == LAST, m == LAST)))
        def _():
            arrived(gy.at[m], rs.at[0, m])
            arrived(carry.at[m], rs.at[1, m])

        g = gy[m].reshape(FEATS, ROWS)
        for i in range(XS):
            d1s[m, i] = jnp.dot(wd_v[(1 - core) * XS + i], g, preferred_element_type=f32).astype(bf16)
        remote(d1s.at[m], d1r.at[m], ss.at[2, m], rs.at[2, m], (s, mate, c)).start()
        for i in range(XS):
            own[m, i] = jnp.dot(wd_v[core * XS + i], g, preferred_element_type=f32)

    def halved(m):
        arrived(d1r.at[m], rs.at[2, m])
        for k in FAR_X:
            to = at_x(k)
            xsd[m, to] = (own[m, to] + d1r[m, to].astype(f32)).astype(bf16)
            remote(xsd.at[m, to], xrv.at[m, x], ss.at[3, m], rs.at[3, m], (s, 2 * to + core, c)).start()
        mine[m] = own[m, x] + d1r[m, x].astype(f32)

    def summed(m):
        arrived(xrv.at[m, pl.ds(0, XS - 1)], rs.at[3, m])
        total = mine[m]
        for k in FAR_X:
            total = total + xrv[m, at_x(k)].astype(f32)
        ga[m, core, x] = total.astype(bf16)
        for k in FAR_X:
            remote(ga.at[m, core, x], ga.at[m, core, x], ss.at[4, m], rs.at[4, m], (s, 2 * at_x(k) + core, c)).start()

    def gradients(m, half):
        g = ga[m, half].reshape(HALF, ROWS).astype(f32)
        grads[0] = (g * slope[m, 0, half]).astype(bf16)
        grads[1] = (g * slope[m, 1, half]).astype(bf16)

    def spread(m):
        arrived(ga.at[m, core, pl.ds(0, XS - 1)], rs.at[4, m])
        remote(ga.at[m, core], ga.at[m, core], ss.at[5, m], rs.at[5, m], (s, mate, c)).start()
        gradients(m, core)
        for b in range(2):
            rows = pl.ds(b * 256, 256)
            acc[rows] = jnp.dot(wg_v[core, rows], grads[0], preferred_element_type=f32) + jnp.dot(
                wu_v[core, rows], grads[1], preferred_element_type=f32
            )

    def features(m):
        other = 1 - core
        arrived(ga.at[m, other], rs.at[5, m])
        gradients(m, other)
        inner = jnp.zeros((1, ROWS), f32)
        for b in range(2):
            rows = pl.ds(b * 256, 256)
            part = (
                acc[rows]
                + jnp.dot(wg_v[other, rows], grads[0], preferred_element_type=f32)
                + jnp.dot(wu_v[other, rows], grads[1], preferred_element_type=f32)
            )
            scaled = gx[pl.ds(4 * b, 4), m].reshape(256, ROWS).astype(f32)
            inner = inner + jnp.sum(part * scaled, axis=0, keepdims=True)
            zs[m, pl.ds(4 * b, 4)] = part.astype(bf16).reshape(4, CHUNK, ROWS)
        for k in FAR_Z:
            to = at_col(k)
            remote(zs.at[m, to], zr.at[m, c], ss.at[6, m], rs.at[6, m], (s, r, to)).start()
        zr[m, c] = zs[m, c]
        ixs[m] = inner
        ixr[m, r] = inner
        for k in range(1, ROW):
            remote(ixs.at[m], ixr.at[m, r], ss.at[7, m], rs.at[7, m], (s, lax.rem(r + k, ROW), c)).start()

    def projected(m):
        arrived(ixr.at[m, pl.ds(0, ROW - 1)], rs.at[7, m])
        inner = jnp.sum(ixr[m], axis=0)
        izs[m] = inner
        izr[m, c] = inner
        for k in FAR_Z:
            remote(izs.at[m], izr.at[m, c], ss.at[8, m], rs.at[8, m], (s, r, at_col(k))).start()

    def updated(m):
        arrived(zr.at[m, pl.ds(0, COL - 1)], rs.at[6, m])
        arrived(izr.at[m, pl.ds(0, COL - 1)], rs.at[8, m])
        total = jnp.sum(zr[m].astype(f32), axis=0)
        inner = jnp.sum(izr[m], axis=0) / D
        root = rstd[m]
        fresh = carry[m] + root * (gain_t[...] * total) - x_t[m] * (root * root * root) * inner
        after[m] = fresh

        @pl.when(s != 0)
        def _():
            gys[m] = fresh.astype(bf16)
            for k in (*FAR_Z, 0):
                remote(gys.at[m], gy.at[m, c], ss.at[0, m], rs.at[0, m], (s - 1, r, at_col(k))).start()
            remote(after.at[m], carry.at[m], ss.at[1, m], rs.at[1, m], (s - 1, r, c)).start()

        @pl.when(jnp.logical_and(s == 0, m != 0))
        def _():
            remote(after.at[m], home, ss.at[1, m], one_r.at[4], (m, r, c)).start()

        @pl.when(jnp.logical_and(s == 0, m == 0))
        def _():
            home[...] = fresh

    def squares_met():
        arrived(sqz.at[pl.ds(0, COL - 1)], one_r.at[2])
        total = jnp.sum(sqz[...], axis=0)
        sqm[...] = total
        sqx[r] = total
        for k in range(1, ROW):
            remote(sqm, sqx.at[r], one_s.at[3], one_r.at[3], (s, lax.rem(r + k, ROW), c)).start()

    def roots():
        arrived(sqx.at[pl.ds(0, ROW - 1)], one_r.at[3])
        arrived(gx.at[pl.ds(0, COL - 1)], one_r.at[1])
        root = lax.rsqrt(jnp.sum(sqx[...], axis=0) / D + eps)
        for m in range(MB):
            rstd[m] = root[m : m + 1]

    def slot(t, carry_):
        def stage(lag, body):
            @pl.when(jnp.logical_and(t >= lag, t < lag + MB))
            def _():
                body(LAST - (t - lag))

        stage(0, hidden)

        @pl.when(t == 0)
        def _():
            squares_met()

        stage(2, spread)
        stage(1, summed)
        stage(0, halved)

        @pl.when(jnp.logical_and(s == LAST, t < LAST))
        def _():
            slopes(LAST - 1 - t)

        @pl.when(t == 1)
        def _():
            roots()

        stage(2, features)
        stage(3, updated)
        stage(2, projected)
        return carry_

    lax.fori_loop(0, SLOTS, slot, 0)

    @pl.when(s == LAST)
    def _():
        epilogue_inputs()

    @pl.when(s != 0)
    def _():
        arrived(home, one_r.at[4])

    resid = home[...] + inc_t[...] - cot_t[...]
    res_o[...] = resid
    part = jnp.concatenate([jnp.sum(v_t[i] * resid, axis=0, keepdims=True) for i in range(UPD)], axis=0)
    dxs[...] = part
    dxr[r] = part
    for k in range(1, ROW):
        remote(dxs, dxr.at[r], one_s.at[5], one_r.at[5], (s, lax.rem(r + k, ROW), c)).start()
    arrived(dxr.at[pl.ds(0, ROW - 1)], one_r.at[5])
    part = jnp.sum(dxr[...], axis=0)
    dzs[...] = part
    dzr[c] = part
    for k in FAR_Z:
        remote(dzs, dzr.at[c], one_s.at[6], one_r.at[6], (s, r, at_col(k))).start()
    arrived(dzr.at[pl.ds(0, COL - 1)], one_r.at[6])
    dots = jnp.sum(jnp.sum(dzr[...], axis=0), axis=1, keepdims=True)
    update = dots[0:1] * u_t[0]
    for i in range(1, UPD):
        update = update + dots[i : i + 1] * u_t[i]
    new_o[...] = cot_t[...] + resid - update

    @pl.when(s == LAST)
    def _():
        left(gy.at[0, pl.ds(0, COL - 1)], first.at[0])

    @pl.when(s != LAST)
    def _():
        left(gy.at[0], first.at[0])
        left(cot_t, first.at[1])

    left(gx.at[pl.ds(0, COL - 1)], one_s.at[1])
    left(sqz.at[pl.ds(0, COL - 1)], one_s.at[2])
    left(sqx.at[pl.ds(0, ROW - 1)], one_s.at[3])
    left(dxr.at[pl.ds(0, ROW - 1)], one_s.at[5])
    left(dzr.at[pl.ds(0, COL - 1)], one_s.at[6])

    def drained(m, carry_):
        @pl.when(s != 0)
        def _():
            left(gy.at[m], ss.at[0, m])

        @pl.when(jnp.logical_or(s != 0, m != 0))
        def _():
            left(after.at[m], ss.at[1, m])

        left(d1s.at[m], ss.at[2, m])
        left(xrv.at[m, pl.ds(0, XS - 1)], ss.at[3, m])
        left(ga.at[m, core, pl.ds(0, XS - 1)], ss.at[4, m])
        left(ga.at[m, core], ss.at[5, m])
        left(zr.at[m, pl.ds(0, COL - 1)], ss.at[6, m])
        left(ixr.at[m, pl.ds(0, ROW - 1)], ss.at[7, m])
        left(izr.at[m, pl.ds(0, COL - 1)], ss.at[8, m])
        return carry_

    lax.fori_loop(0, MB, drained, 0)


def shards(cotangent, incoming, upd_u, upd_v, saved_x, saved_h, norm_gain, w_gate, w_up, w_down):
    vm = pltpu.VMEM
    dma = pltpu.SemaphoreType.DMA
    tile = (CHUNK, ROWS)
    new, res = pl.pallas_call(
        kernel,
        out_shape=[jax.ShapeDtypeStruct(tile, f32)] * 2,
        in_specs=[pl.BlockSpec(memory_space=pl.ANY)] * 10,
        out_specs=[pl.BlockSpec(memory_space=pltpu.VMEM)] * 2,
        scratch_shapes=[
            vm((ROWS, CHUNK), f32),
            vm((ROWS, CHUNK), f32),
            vm((UPD, ROWS, CHUNK), f32),
            vm((UPD, ROWS, CHUNK), f32),
            vm((MB, ROWS, CHUNK), bf16),
            vm((MB, 2, ROWS, HID), bf16),
            vm((1, CHUNK), f32),
            vm((2, FEATS, HALF), bf16),
            vm((2, FEATS, HALF), bf16),
            vm((ROW, PIECE, FEATS), bf16),
            vm(tile, f32),
            vm(tile, f32),
            vm((UPD, *tile), f32),
            vm((UPD, *tile), f32),
            vm((MB, *tile), f32),
            vm(tile, f32),
            vm((COL, MB, *tile), bf16),
            vm((MB, 2, 2, HALF, ROWS), f32),
            vm(tile, bf16),
            vm((MB, COL, *tile), bf16),
            vm((MB, *tile), bf16),
            vm((MB, *tile), f32),
            vm((MB, *tile), f32),
            vm((MB, XS, PIECE, ROWS), bf16),
            vm((MB, XS, PIECE, ROWS), bf16),
            vm((MB, XS, PIECE, ROWS), f32),
            vm((MB, XS, PIECE, ROWS), bf16),
            vm((MB, XS, PIECE, ROWS), bf16),
            vm((MB, PIECE, ROWS), f32),
            vm((MB, 2, XS, PIECE, ROWS), bf16),
            vm((2, HALF, ROWS), bf16),
            vm((FEATS, ROWS), f32),
            vm((MB, COL, *tile), bf16),
            vm((MB, COL, *tile), bf16),
            vm((MB, 1, ROWS), f32),
            vm((MB, ROW, 1, ROWS), f32),
            vm((MB, 1, ROWS), f32),
            vm((MB, COL, 1, ROWS), f32),
            vm((8, ROWS), f32),
            vm((COL, 8, ROWS), f32),
            vm((8, ROWS), f32),
            vm((ROW, 8, ROWS), f32),
            vm((MB, 1, ROWS), f32),
            vm(tile, f32),
            vm((UPD, ROWS), f32),
            vm((ROW, UPD, ROWS), f32),
            vm((UPD, ROWS), f32),
            vm((COL, UPD, ROWS), f32),
            dma((12,)),
            dma((2,)),
            dma((9, MB)),
            dma((9, MB)),
            dma((7,)),
            dma((7,)),
        ],
        compiler_params=pltpu.CompilerParams(
            collective_id=0, has_side_effects=True, vmem_limit_bytes=60 * 1024 * 1024
        ),
        name="broyden",
    )(
        cotangent, incoming, upd_u, upd_v, saved_x, saved_h, norm_gain,
        w_gate, w_up, w_down.reshape(1, ROW, PIECE, FEATS),
    )
    return new.T[None], res.T[None]


def solution(mesh):
    placed = (
        P("section", None, ("row", "col")),
        P("section", None, ("row", "col")),
        P("section", None, None, ("row", "col")),
        P("section", None, None, ("row", "col")),
        P("section", None, None, ("row", "col")),
        P("section", None, None, None, "col"),
        P("section", ("row", "col")),
        P("section", "row", "col"),
        P("section", "row", "col"),
        P("section", "col", "row"),
    )
    return jax.shard_map(
        shards,
        mesh=mesh,
        in_specs=placed,
        out_specs=(P("section", None, ("row", "col")), P("section", None, ("row", "col"))),
        check_vma=False,
    )
```

```python
import jax
import jax.numpy as jnp
from jax import lax
from jax.experimental import pallas as pl
from jax.experimental.pallas import tpu as pltpu
from jax.sharding import PartitionSpec as P

D = 4096
FF = 14336
ROWS = 128
UPD = 8
MB = 4
SECTIONS, ROW, COL = 4, 8, 8
XS = ROW // 2
CHUNK = D // (ROW * COL)
FEATS = D // ROW
HID = FF // COL
HALF = HID // 2
PIECE = HID // ROW
FAR_Z = (4, 3, 5, 2, 6, 1, 7)
FAR_X = (2, 1, 3)
SLOTS = MB + 3

eps = 1e-05
bf16 = jnp.bfloat16
f32 = jnp.float32
MESH = pl.DeviceIdType.MESH


def kernel(
    cot_h, inc_h, u_h, v_h, x_h, h_h, gain_h, wg_h, wu_h, wd_h,
    new_o, res_o,
    cot_t, inc_t, u_t, v_t, x_v, h_v, gain_v, wg_v, wu_v, wd_v,
    x_t, gain_t, gx, slope,
    start, gy, gys, carry, after, d1s, d1r, own, xsd, xrv, mine, ga, grads, acc, zs, zr,
    ixs, ixr, izs, izr, sqs, sqz, sqm, sqx, rstd, home, dxs, dxr, dzs, dzr,
    load, first, ss, rs, one_s, one_r,
):
    s = lax.axis_index("section")
    r = lax.axis_index("row")
    c = lax.axis_index("col")
    core = lax.rem(r, 2)
    x = lax.div(r, 2)
    mate = r + 1 - 2 * core

    def at_col(k):
        return lax.rem(c + k, COL)

    def at_x(k):
        return lax.rem(x + k, XS)

    def remote(src, dst, send, recv, device):
        return pltpu.make_async_remote_copy(
            src_ref=src, dst_ref=dst, send_sem=send, recv_sem=recv, device_id=device, device_id_type=MESH
        )

    def arrived(ref, recv):
        remote(ref, ref, one_s.at[0], recv, (s, mate, c)).wait_recv()

    def left(ref, send):
        remote(ref, ref, send, one_r.at[0], (s, mate, c)).wait_send()

    loads = {}
    for i, (name, src, dst) in enumerate(
        (
            ("cot", cot_h.at[0], cot_t),
            ("gain", gain_h, gain_v),
            ("x", x_h.at[0], x_v),
            ("wd", wd_h.at[0], wd_v),
            ("h", h_h.at[0], h_v),
            ("wg0", wg_h.at[0, :, pl.ds(0, HALF)], wg_v.at[0]),
            ("wg1", wg_h.at[0, :, pl.ds(HALF, HALF)], wg_v.at[1]),
            ("wu0", wu_h.at[0, :, pl.ds(0, HALF)], wu_v.at[0]),
            ("wu1", wu_h.at[0, :, pl.ds(HALF, HALF)], wu_v.at[1]),
            ("inc", inc_h.at[0], inc_t),
            ("u", u_h.at[0], u_t),
            ("v", v_h.at[0], v_t),
        )
    ):
        loads[name] = pltpu.make_async_copy(src, dst, load.at[i])
        loads[name].start()

    barrier = pltpu.get_barrier_semaphore()
    for ds in range(SECTIONS):
        for dc in range(COL):
            if ds or dc:
                there = (lax.rem(s + ds, SECTIONS), r, at_col(dc))
                pl.semaphore_signal(barrier, inc=1, device_id=there, device_id_type=MESH)
    for dr in range(1, ROW):
        pl.semaphore_signal(barrier, inc=1, device_id=(s, lax.rem(r + dr, ROW), c), device_id_type=MESH)

    loads["cot"].wait()
    start[...] = cot_t[...].astype(bf16)
    pl.semaphore_wait(barrier, SECTIONS * COL - 1 + ROW - 1)

    LAST = SECTIONS - 1
    mb_home = s

    @pl.when(s == LAST)
    def _():
        gy[LAST, c] = start[...]
        carry[LAST] = cot_t[...]
        for k in FAR_Z:
            remote(start, gy.at[LAST, c], first.at[0], rs.at[0, LAST], (LAST, r, at_col(k))).start()

    @pl.when(s != LAST)
    def _():
        for k in (*FAR_Z, 0):
            remote(start, gy.at[mb_home, c], first.at[0], rs.at[0, mb_home], (LAST, r, at_col(k))).start()
        remote(cot_t, carry.at[mb_home], first.at[1], rs.at[1, mb_home], (LAST, r, c)).start()

    loads["gain"].wait()
    loads["x"].wait()
    gain_t[...] = jnp.broadcast_to(gain_v[...], (ROWS, CHUNK)).T
    sums = []
    for m in range(MB):
        xt = x_v[m].astype(f32)
        x_t[m] = xt
        gx[c, m] = (gain_t[...] * xt).astype(bf16)
        sums.append(jnp.sum(xt * xt, axis=0, keepdims=True))
    sums = jnp.concatenate(sums + sums, axis=0)
    sqs[...] = sums
    sqz[c] = sums
    for k in FAR_Z:
        remote(gx.at[c], gx.at[c], one_s.at[1], one_r.at[1], (s, r, at_col(k))).start()
        remote(sqs, sqz.at[c], one_s.at[2], one_r.at[2], (s, r, at_col(k))).start()

    def slopes(m):
        for half in range(2):
            for b in range(7):
                at = pl.ds(half * HALF + b * 128, 128)
                hg = h_v[m, 0, :, at].astype(f32)
                hu = h_v[m, 1, :, at].astype(f32)
                sig = jax.nn.sigmoid(hg)
                slope[m, 0, half, pl.ds(b * 128, 128)] = (hu * sig * (1.0 + hg * (1.0 - sig))).T
                slope[m, 1, half, pl.ds(b * 128, 128)] = (hg * sig).T

    loads["h"].wait()
    loads["inc"].wait()
    loads["u"].wait()
    loads["v"].wait()

    @pl.when(s != LAST)
    def _():
        def body(m, carry_):
            slopes(m)
            return carry_

        lax.fori_loop(0, MB, body, 0)

    @pl.when(s == LAST)
    def _():
        slopes(LAST)

    for name in ("wd", "wg0", "wg1", "wu0", "wu1"):
        loads[name].wait()

    def hidden(m):
        @pl.when(jnp.logical_and(s == LAST, m == LAST))
        def _():
            arrived(gy.at[m, pl.ds(0, COL - 1)], rs.at[0, m])

        @pl.when(jnp.logical_not(jnp.logical_and(s == LAST, m == LAST)))
        def _():
            arrived(gy.at[m], rs.at[0, m])
            arrived(carry.at[m], rs.at[1, m])

        g = gy[m].reshape(FEATS, ROWS)
        for i in range(XS):
            d1s[m, i] = jnp.dot(wd_v[(1 - core) * XS + i], g, preferred_element_type=f32).astype(bf16)
        remote(d1s.at[m], d1r.at[m], ss.at[2, m], rs.at[2, m], (s, mate, c)).start()
        for i in range(XS):
            own[m, i] = jnp.dot(wd_v[core * XS + i], g, preferred_element_type=f32)

    def halved(m):
        arrived(d1r.at[m], rs.at[2, m])
        for k in FAR_X:
            to = at_x(k)
            xsd[m, to] = (own[m, to] + d1r[m, to].astype(f32)).astype(bf16)
            remote(xsd.at[m, to], xrv.at[m, x], ss.at[3, m], rs.at[3, m], (s, 2 * to + core, c)).start()
        mine[m] = own[m, x] + d1r[m, x].astype(f32)

    def summed(m):
        arrived(xrv.at[m, pl.ds(0, XS - 1)], rs.at[3, m])
        total = mine[m]
        for k in FAR_X:
            total = total + xrv[m, at_x(k)].astype(f32)
        ga[m, core, x] = total.astype(bf16)
        for k in FAR_X:
            remote(ga.at[m, core, x], ga.at[m, core, x], ss.at[4, m], rs.at[4, m], (s, 2 * at_x(k) + core, c)).start()

    def gradients(m, half):
        g = ga[m, half].reshape(HALF, ROWS).astype(f32)
        grads[0] = (g * slope[m, 0, half]).astype(bf16)
        grads[1] = (g * slope[m, 1, half]).astype(bf16)

    def spread(m):
        arrived(ga.at[m, core, pl.ds(0, XS - 1)], rs.at[4, m])
        remote(ga.at[m, core], ga.at[m, core], ss.at[5, m], rs.at[5, m], (s, mate, c)).start()
        gradients(m, core)
        for b in range(2):
            rows = pl.ds(b * 256, 256)
            acc[rows] = jnp.dot(wg_v[core, rows], grads[0], preferred_element_type=f32) + jnp.dot(
                wu_v[core, rows], grads[1], preferred_element_type=f32
            )

    def features(m):
        other = 1 - core
        arrived(ga.at[m, other], rs.at[5, m])
        gradients(m, other)
        inner = jnp.zeros((1, ROWS), f32)
        for b in range(2):
            rows = pl.ds(b * 256, 256)
            part = (
                acc[rows]
                + jnp.dot(wg_v[other, rows], grads[0], preferred_element_type=f32)
                + jnp.dot(wu_v[other, rows], grads[1], preferred_element_type=f32)
            )
            scaled = gx[pl.ds(4 * b, 4), m].reshape(256, ROWS).astype(f32)
            inner = inner + jnp.sum(part * scaled, axis=0, keepdims=True)
            zs[m, pl.ds(4 * b, 4)] = part.astype(bf16).reshape(4, CHUNK, ROWS)
        for k in FAR_Z:
            to = at_col(k)
            remote(zs.at[m, to], zr.at[m, c], ss.at[6, m], rs.at[6, m], (s, r, to)).start()
        zr[m, c] = zs[m, c]
        ixs[m] = inner
        ixr[m, r] = inner
        for k in range(1, ROW):
            remote(ixs.at[m], ixr.at[m, r], ss.at[7, m], rs.at[7, m], (s, lax.rem(r + k, ROW), c)).start()

    def projected(m):
        arrived(ixr.at[m, pl.ds(0, ROW - 1)], rs.at[7, m])
        inner = jnp.sum(ixr[m], axis=0)
        izs[m] = inner
        izr[m, c] = inner
        for k in FAR_Z:
            remote(izs.at[m], izr.at[m, c], ss.at[8, m], rs.at[8, m], (s, r, at_col(k))).start()

    def updated(m):
        arrived(zr.at[m, pl.ds(0, COL - 1)], rs.at[6, m])
        arrived(izr.at[m, pl.ds(0, COL - 1)], rs.at[8, m])
        total = jnp.sum(zr[m].astype(f32), axis=0)
        inner = jnp.sum(izr[m], axis=0) / D
        root = rstd[m]
        fresh = carry[m] + root * (gain_t[...] * total) - x_t[m] * (root * root * root) * inner
        after[m] = fresh

        @pl.when(s != 0)
        def _():
            gys[m] = fresh.astype(bf16)
            for k in (*FAR_Z, 0):
                remote(gys.at[m], gy.at[m, c], ss.at[0, m], rs.at[0, m], (s - 1, r, at_col(k))).start()
            remote(after.at[m], carry.at[m], ss.at[1, m], rs.at[1, m], (s - 1, r, c)).start()

        @pl.when(jnp.logical_and(s == 0, m != 0))
        def _():
            remote(after.at[m], home, ss.at[1, m], one_r.at[4], (m, r, c)).start()

        @pl.when(jnp.logical_and(s == 0, m == 0))
        def _():
            home[...] = fresh

    def squares_met():
        arrived(sqz.at[pl.ds(0, COL - 1)], one_r.at[2])
        total = jnp.sum(sqz[...], axis=0)
        sqm[...] = total
        sqx[r] = total
        for k in range(1, ROW):
            remote(sqm, sqx.at[r], one_s.at[3], one_r.at[3], (s, lax.rem(r + k, ROW), c)).start()

    def roots():
        arrived(sqx.at[pl.ds(0, ROW - 1)], one_r.at[3])
        arrived(gx.at[pl.ds(0, COL - 1)], one_r.at[1])
        root = lax.rsqrt(jnp.sum(sqx[...], axis=0) / D + eps)
        for m in range(MB):
            rstd[m] = root[m : m + 1]

    def slot(t, carry_):
        def stage(lag, body):
            @pl.when(jnp.logical_and(t >= lag, t < lag + MB))
            def _():
                body(LAST - (t - lag))

        stage(0, hidden)

        @pl.when(t == 0)
        def _():
            squares_met()

        stage(2, spread)
        stage(1, summed)
        stage(0, halved)

        @pl.when(jnp.logical_and(s == LAST, t < LAST))
        def _():
            slopes(LAST - 1 - t)

        @pl.when(t == 1)
        def _():
            roots()

        stage(2, features)
        stage(3, updated)
        stage(2, projected)
        return carry_

    lax.fori_loop(0, SLOTS, slot, 0)

    @pl.when(s != 0)
    def _():
        arrived(home, one_r.at[4])

    resid = home[...] + inc_t[...] - cot_t[...]
    res_o[...] = resid
    part = jnp.concatenate([jnp.sum(v_t[i] * resid, axis=0, keepdims=True) for i in range(UPD)], axis=0)
    dxs[...] = part
    dxr[r] = part
    for k in range(1, ROW):
        remote(dxs, dxr.at[r], one_s.at[5], one_r.at[5], (s, lax.rem(r + k, ROW), c)).start()
    arrived(dxr.at[pl.ds(0, ROW - 1)], one_r.at[5])
    part = jnp.sum(dxr[...], axis=0)
    dzs[...] = part
    dzr[c] = part
    for k in FAR_Z:
        remote(dzs, dzr.at[c], one_s.at[6], one_r.at[6], (s, r, at_col(k))).start()
    arrived(dzr.at[pl.ds(0, COL - 1)], one_r.at[6])
    dots = jnp.sum(jnp.sum(dzr[...], axis=0), axis=1, keepdims=True)
    update = dots[0:1] * u_t[0]
    for i in range(1, UPD):
        update = update + dots[i : i + 1] * u_t[i]
    new_o[...] = cot_t[...] + resid - update

    @pl.when(s == LAST)
    def _():
        left(gy.at[0, pl.ds(0, COL - 1)], first.at[0])

    @pl.when(s != LAST)
    def _():
        left(gy.at[0], first.at[0])
        left(cot_t, first.at[1])

    left(gx.at[pl.ds(0, COL - 1)], one_s.at[1])
    left(sqz.at[pl.ds(0, COL - 1)], one_s.at[2])
    left(sqx.at[pl.ds(0, ROW - 1)], one_s.at[3])
    left(dxr.at[pl.ds(0, ROW - 1)], one_s.at[5])
    left(dzr.at[pl.ds(0, COL - 1)], one_s.at[6])

    def drained(m, carry_):
        @pl.when(s != 0)
        def _():
            left(gy.at[m], ss.at[0, m])

        @pl.when(jnp.logical_or(s != 0, m != 0))
        def _():
            left(after.at[m], ss.at[1, m])

        left(d1s.at[m], ss.at[2, m])
        left(xrv.at[m, pl.ds(0, XS - 1)], ss.at[3, m])
        left(ga.at[m, core, pl.ds(0, XS - 1)], ss.at[4, m])
        left(ga.at[m, core], ss.at[5, m])
        left(zr.at[m, pl.ds(0, COL - 1)], ss.at[6, m])
        left(ixr.at[m, pl.ds(0, ROW - 1)], ss.at[7, m])
        left(izr.at[m, pl.ds(0, COL - 1)], ss.at[8, m])
        return carry_

    lax.fori_loop(0, MB, drained, 0)


def turned(a):
    return jnp.swapaxes(a, -1, -2)


def shards(cotangent, incoming, upd_u, upd_v, saved_x, saved_h, norm_gain, w_gate, w_up, w_down):
    vm = pltpu.VMEM
    dma = pltpu.SemaphoreType.DMA
    tile = (CHUNK, ROWS)
    new, res = pl.pallas_call(
        kernel,
        out_shape=[jax.ShapeDtypeStruct(tile, f32)] * 2,
        in_specs=[pl.BlockSpec(memory_space=pl.ANY)] * 10,
        out_specs=[pl.BlockSpec(memory_space=pltpu.VMEM)] * 2,
        scratch_shapes=[
            vm(tile, f32),
            vm(tile, f32),
            vm((UPD, *tile), f32),
            vm((UPD, *tile), f32),
            vm((MB, *tile), bf16),
            vm((MB, 2, ROWS, HID), bf16),
            vm((1, CHUNK), f32),
            vm((2, FEATS, HALF), bf16),
            vm((2, FEATS, HALF), bf16),
            vm((ROW, PIECE, FEATS), bf16),
            vm((MB, *tile), f32),
            vm(tile, f32),
            vm((COL, MB, *tile), bf16),
            vm((MB, 2, 2, HALF, ROWS), f32),
            vm(tile, bf16),
            vm((MB, COL, *tile), bf16),
            vm((MB, *tile), bf16),
            vm((MB, *tile), f32),
            vm((MB, *tile), f32),
            vm((MB, XS, PIECE, ROWS), bf16),
            vm((MB, XS, PIECE, ROWS), bf16),
            vm((MB, XS, PIECE, ROWS), f32),
            vm((MB, XS, PIECE, ROWS), bf16),
            vm((MB, XS, PIECE, ROWS), bf16),
            vm((MB, PIECE, ROWS), f32),
            vm((MB, 2, XS, PIECE, ROWS), bf16),
            vm((2, HALF, ROWS), bf16),
            vm((FEATS, ROWS), f32),
            vm((MB, COL, *tile), bf16),
            vm((MB, COL, *tile), bf16),
            vm((MB, 1, ROWS), f32),
            vm((MB, ROW, 1, ROWS), f32),
            vm((MB, 1, ROWS), f32),
            vm((MB, COL, 1, ROWS), f32),
            vm((8, ROWS), f32),
            vm((COL, 8, ROWS), f32),
            vm((8, ROWS), f32),
            vm((ROW, 8, ROWS), f32),
            vm((MB, 1, ROWS), f32),
            vm(tile, f32),
            vm((UPD, ROWS), f32),
            vm((ROW, UPD, ROWS), f32),
            vm((UPD, ROWS), f32),
            vm((COL, UPD, ROWS), f32),
            dma((12,)),
            dma((2,)),
            dma((9, MB)),
            dma((9, MB)),
            dma((7,)),
            dma((7,)),
        ],
        compiler_params=pltpu.CompilerParams(
            collective_id=0, has_side_effects=True, vmem_limit_bytes=60 * 1024 * 1024
        ),
        name="broyden",
    )(
        turned(cotangent), turned(incoming), turned(upd_u), turned(upd_v), turned(saved_x), saved_h, norm_gain,
        w_gate, w_up, w_down.reshape(1, ROW, PIECE, FEATS),
    )
    return new.T[None], res.T[None]


def solution(mesh):
    placed = (
        P("section", None, ("row", "col")),
        P("section", None, ("row", "col")),
        P("section", None, None, ("row", "col")),
        P("section", None, None, ("row", "col")),
        P("section", None, None, ("row", "col")),
        P("section", None, None, None, "col"),
        P("section", ("row", "col")),
        P("section", "row", "col"),
        P("section", "row", "col"),
        P("section", "col", "row"),
    )
    return jax.shard_map(
        shards,
        mesh=mesh,
        in_specs=placed,
        out_specs=(P("section", None, ("row", "col")), P("section", None, ("row", "col"))),
        check_vma=False,
    )
```

```python
import jax
import jax.numpy as jnp
from jax import lax
from jax.experimental import pallas as pl
from jax.experimental.pallas import tpu as pltpu
from jax.sharding import PartitionSpec as P

D = 4096
FF = 14336
ROWS = 128
UPD = 8
MB = 4
SECTIONS, ROW, COL = 4, 8, 8
XS = ROW // 2
CHUNK = D // (ROW * COL)
FEATS = D // ROW
HID = FF // COL
HALF = HID // 2
PIECE = HID // ROW
FAR_Z = (4, 3, 5, 2, 6, 1, 7)
FAR_X = (2, 1, 3)
ORDER = [
    ("H", 3), ("V", 3), ("S", 3), ("H", 2), ("V", 2), ("q", 0), ("P", 3), ("g", 0), ("F", 3), ("S", 2),
    ("H", 1), ("V", 1), ("r", 0), ("U", 3), ("P", 2), ("F", 2), ("S", 1), ("H", 0), ("V", 0), ("U", 2),
    ("P", 1), ("F", 1), ("S", 0), ("U", 1), ("P", 0), ("F", 0), ("U", 0),
]

eps = 1e-05
bf16 = jnp.bfloat16
f32 = jnp.float32
MESH = pl.DeviceIdType.MESH


def kernel(
    cot_h, inc_h, u_h, v_h, x_h, h_h, gain_h, wg_h, wu_h, wd_h,
    new_o, res_o,
    cot_t, inc_t, u_t, v_t, x_v, h_v, gain_v, wg_v, wu_v, wd_v,
    x_t, gain_t, gx, slope,
    start, gy, gys, carry, after, d1s, d1r, own, xsd, xrv, mine, ga, grads, acc, zs, zr,
    kzs, kzr, kps, kpr, above, above_all, lean, below, sqs, sqz, sqm, sqx, rstd, home, khome, vxs, vxr, vzs, vzr, dxs, dxr, dzs, dzr,
    load, first, ss, rs, one_s, one_r,
):
    s = lax.axis_index("section")
    r = lax.axis_index("row")
    c = lax.axis_index("col")
    core = lax.rem(r, 2)
    x = lax.div(r, 2)
    mate = r + 1 - 2 * core

    def at_col(k):
        return lax.rem(c + k, COL)

    def at_x(k):
        return lax.rem(x + k, XS)

    def remote(src, dst, send, recv, device):
        return pltpu.make_async_remote_copy(
            src_ref=src, dst_ref=dst, send_sem=send, recv_sem=recv, device_id=device, device_id_type=MESH
        )

    def arrived(ref, recv):
        remote(ref, ref, one_s.at[0], recv, (s, mate, c)).wait_recv()

    def left(ref, send):
        remote(ref, ref, send, one_r.at[0], (s, mate, c)).wait_send()

    barrier = pltpu.get_barrier_semaphore()
    for k in FAR_Z:
        pl.semaphore_signal(barrier, inc=1, device_id=(s, r, at_col(k)), device_id_type=MESH)
    for k in (2, 1, 3):
        pl.semaphore_signal(barrier, inc=1, device_id=(lax.rem(s + k, SECTIONS), r, c), device_id_type=MESH)
    for k in range(1, ROW):
        pl.semaphore_signal(barrier, inc=1, device_id=(s, lax.rem(r + k, ROW), c), device_id_type=MESH)

    loads = {}
    for i, (name, src, dst) in enumerate(
        (
            ("cot", cot_h.at[0], cot_t),
            ("gain", gain_h, gain_v),
            ("x", x_h.at[0], x_v),
            ("wd", wd_h.at[0], wd_v),
            ("h", h_h.at[0], h_v),
            ("wg0", wg_h.at[0, :, pl.ds(0, HALF)], wg_v.at[0]),
            ("wg1", wg_h.at[0, :, pl.ds(HALF, HALF)], wg_v.at[1]),
            ("wu0", wu_h.at[0, :, pl.ds(0, HALF)], wu_v.at[0]),
            ("wu1", wu_h.at[0, :, pl.ds(HALF, HALF)], wu_v.at[1]),
            ("inc", inc_h.at[0], inc_t),
            ("u", u_h.at[0], u_t),
            ("v", v_h.at[0], v_t),
        )
    ):
        loads[name] = pltpu.make_async_copy(src, dst, load.at[i])
        loads[name].start()

    loads["cot"].wait()
    start[...] = cot_t[...].astype(bf16)
    pl.semaphore_wait(barrier, SECTIONS - 1 + COL - 1 + ROW - 1)

    LAST = SECTIONS - 1
    mb_home = s

    @pl.when(s == LAST)
    def _():
        gy[LAST, c] = start[...]
        carry[LAST] = cot_t[...]
        for k in FAR_Z:
            remote(
                start, gy.at[LAST, c], first.at[0], rs.at[0, LAST], (LAST, r, at_col(k))
            ).start()

    loads["x"].wait()

    @pl.when(s != 0)
    def _():
        remote(x_v, above, one_s.at[7], one_r.at[7], (s - 1, r, c)).start()

    @pl.when(s == 0)
    def _():
        for m in range(1, MB):
            remote(x_v.at[m], below, one_s.at[8], one_r.at[8], (m, r, c)).start()
        below[...] = x_v[0]

    loads["gain"].wait()
    gain_t[...] = jnp.broadcast_to(gain_v[...], (ROWS, CHUNK)).T
    sums = []
    for m in range(MB):
        xt = x_v[m].astype(f32)
        x_t[m] = xt
        gx[c, m] = (gain_t[...] * xt).astype(bf16)
        sums.append(jnp.sum(xt * xt, axis=0, keepdims=True))
    sums = jnp.concatenate(sums + sums, axis=0)
    sqs[...] = sums
    sqz[c] = sums
    for k in FAR_Z:
        remote(sqs, sqz.at[c], one_s.at[2], one_r.at[2], (s, r, at_col(k))).start()

    @pl.when(s != LAST)
    def _():
        arrived(sqz.at[pl.ds(0, COL - 1)], one_r.at[2])
        for k in (*FAR_Z, 0):
            remote(start, gy.at[mb_home, c], first.at[0], rs.at[0, mb_home], (LAST, r, at_col(k))).start()
        remote(cot_t, carry.at[mb_home], first.at[1], rs.at[1, mb_home], (LAST, r, c)).start()
        arrived(above, one_r.at[7])
        above_all[c] = above[...]
        for k in FAR_Z:
            remote(above, above_all.at[c], one_s.at[9], one_r.at[9], (s, r, at_col(k))).start()

    for k in FAR_Z:
        remote(gx.at[c], gx.at[c], one_s.at[1], one_r.at[1], (s, r, at_col(k))).start()

    def slopes(m):
        for half in range(2):
            for b in range(7):
                at = pl.ds(half * HALF + b * 128, 128)
                hg = h_v[m, 0, :, at].astype(f32)
                hu = h_v[m, 1, :, at].astype(f32)
                sig = jax.nn.sigmoid(hg)
                slope[m, 0, half, pl.ds(b * 128, 128)] = (hu * sig * (1.0 + hg * (1.0 - sig))).T
                slope[m, 1, half, pl.ds(b * 128, 128)] = (hg * sig).T

    loads["h"].wait()
    loads["inc"].wait()
    loads["u"].wait()
    loads["v"].wait()

    @pl.when(s != LAST)
    def _():
        def body(m, carry_):
            slopes(m)
            return carry_

        lax.fori_loop(0, MB, body, 0)

    @pl.when(s == LAST)
    def _():
        slopes(LAST)

    for name in ("wd", "wg0", "wg1", "wu0", "wu1"):
        loads[name].wait()

    @pl.when(s != LAST)
    def _():
        arrived(above_all.at[pl.ds(0, COL - 1)], one_r.at[9])

        def body(m, carry_):
            a = above_all[:, m].reshape(FEATS, ROWS)
            for i in range(ROW):
                lean[m, i] = jnp.dot(wd_v[i], a, preferred_element_type=f32)
            return carry_

        lax.fori_loop(0, MB, body, 0)

    def leanings():
        @pl.when(s != 0)
        def _():
            arrived(below, one_r.at[8])

        b = below[...].astype(f32)
        part = jnp.concatenate([jnp.sum(v_t[i] * b, axis=0, keepdims=True) for i in range(UPD)], axis=0)
        vxs[...] = part
        vxr[r] = part
        for k in range(1, ROW):
            remote(vxs, vxr.at[r], one_s.at[11], one_r.at[11], (s, lax.rem(r + k, ROW), c)).start()
        arrived(vxr.at[pl.ds(0, ROW - 1)], one_r.at[11])
        part = jnp.sum(vxr[...], axis=0)
        vzs[...] = part
        vzr[c] = part
        for k in FAR_Z:
            remote(vzs, vzr.at[c], one_s.at[12], one_r.at[12], (s, r, at_col(k))).start()
        arrived(vzr.at[pl.ds(0, COL - 1)], one_r.at[12])

    @pl.when(s != LAST)
    def _():
        leanings()

    def hidden(m):
        @pl.when(s == LAST)
        def _():
            if m == LAST:
                arrived(gy.at[m, pl.ds(0, COL - 1)], rs.at[0, m])
            else:
                arrived(gy.at[m], rs.at[0, m])
                arrived(carry.at[m], rs.at[1, m])
            g = gy[m].reshape(FEATS, ROWS)
            for i in range(XS):
                d1s[m, i] = jnp.dot(wd_v[(1 - core) * XS + i], g, preferred_element_type=f32).astype(bf16)
            remote(d1s.at[m], d1r.at[m], ss.at[2, m], rs.at[2, m], (s, mate, c)).start()
            for i in range(XS):
                own[m, i] = jnp.dot(wd_v[core * XS + i], g, preferred_element_type=f32)

        @pl.when(s != LAST)
        def _():
            arrived(gy.at[m], rs.at[0, m])
            arrived(kpr.at[m], rs.at[7, m])
            arrived(carry.at[m], rs.at[1, m])
            k = jnp.sum(kpr[m], axis=0)
            g = gy[m].reshape(FEATS, ROWS)
            for i in range(XS):
                q = (1 - core) * XS + i
                d1s[m, i] = (jnp.dot(wd_v[q], g, preferred_element_type=f32) - k * lean[m, q]).astype(bf16)
            remote(d1s.at[m], d1r.at[m], ss.at[2, m], rs.at[2, m], (s, mate, c)).start()
            for i in range(XS):
                q = core * XS + i
                own[m, i] = jnp.dot(wd_v[q], g, preferred_element_type=f32) - k * lean[m, q]
            carry[m] = carry[m] - k * above[m].astype(f32)

    def halved(m):
        arrived(d1r.at[m], rs.at[2, m])
        for k in FAR_X:
            to = at_x(k)
            xsd[m, to] = (own[m, to] + d1r[m, to].astype(f32)).astype(bf16)
            remote(xsd.at[m, to], xrv.at[m, x], ss.at[3, m], rs.at[3, m], (s, 2 * to + core, c)).start()
        mine[m] = own[m, x] + d1r[m, x].astype(f32)

    def summed(m):
        arrived(xrv.at[m, pl.ds(0, XS - 1)], rs.at[3, m])
        total = mine[m]
        for k in FAR_X:
            total = total + xrv[m, at_x(k)].astype(f32)
        ga[m, core, x] = total.astype(bf16)
        for k in FAR_X:
            remote(ga.at[m, core, x], ga.at[m, core, x], ss.at[4, m], rs.at[4, m], (s, 2 * at_x(k) + core, c)).start()

    def gradients(m, half):
        g = ga[m, half].reshape(HALF, ROWS).astype(f32)
        grads[0] = (g * slope[m, 0, half]).astype(bf16)
        grads[1] = (g * slope[m, 1, half]).astype(bf16)

    def spread(m):
        arrived(ga.at[m, core, pl.ds(0, XS - 1)], rs.at[4, m])
        remote(ga.at[m, core], ga.at[m, core], ss.at[5, m], rs.at[5, m], (s, mate, c)).start()
        gradients(m, core)
        for b in range(2):
            rows = pl.ds(b * 256, 256)
            acc[rows] = jnp.dot(wg_v[core, rows], grads[0], preferred_element_type=f32) + jnp.dot(
                wu_v[core, rows], grads[1], preferred_element_type=f32
            )

    def features(m):
        other = 1 - core
        arrived(ga.at[m, other], rs.at[5, m])
        gradients(m, other)
        inner = jnp.zeros((1, ROWS), f32)
        for b in range(2):
            rows = pl.ds(b * 256, 256)
            part = (
                acc[rows]
                + jnp.dot(wg_v[other, rows], grads[0], preferred_element_type=f32)
                + jnp.dot(wu_v[other, rows], grads[1], preferred_element_type=f32)
            )
            scaled = gx[pl.ds(4 * b, 4), m].reshape(256, ROWS).astype(f32)
            inner = inner + jnp.sum(part * scaled, axis=0, keepdims=True)
            zs[m, pl.ds(4 * b, 4)] = part.astype(bf16).reshape(4, CHUNK, ROWS)
        for k in FAR_Z:
            to = at_col(k)
            remote(zs.at[m, to], zr.at[m, c], ss.at[6, m], rs.at[6, m], (s, r, to)).start()
        kzs[m] = inner
        for k in FAR_Z:
            remote(kzs.at[m], kzr.at[m, c], ss.at[8, m], rs.at[8, m], (s, r, at_col(k))).start()
        zr[m, c] = zs[m, c]
        kzr[m, c] = inner

    def updated(m):
        arrived(zr.at[m, pl.ds(0, COL - 1)], rs.at[6, m])
        arrived(kzr.at[m, pl.ds(0, COL - 1)], rs.at[8, m])
        total = jnp.sum(zr[m].astype(f32), axis=0)
        inner = jnp.sum(kzr[m], axis=0)
        root = rstd[m]
        fresh = carry[m] + root * (gain_t[...] * total)
        after[m] = fresh
        kps[m] = (root * root * root) * (inner / D)

        @pl.when(s != 0)
        def _():
            gys[m] = fresh.astype(bf16)
            for k in (*FAR_Z, 0):
                remote(
                    gys.at[m], gy.at[m, c], ss.at[0, m], rs.at[0, m], (s - 1, r, at_col(k))
                ).start()
            for k in range(ROW):
                remote(kps.at[m], kpr.at[m, r], ss.at[7, m], rs.at[7, m], (s - 1, lax.rem(r + k, ROW), c)).start()
            remote(after.at[m], carry.at[m], ss.at[1, m], rs.at[1, m], (s - 1, r, c)).start()

        @pl.when(s == 0)
        def _():
            if m == 0:
                home[...] = fresh
                khome[r] = kps[m]
            else:
                remote(after.at[m], home, ss.at[1, m], one_r.at[4], (m, r, c)).start()
            for k in range(1 if m == 0 else 0, ROW):
                remote(kps.at[m], khome.at[r], ss.at[7, m], one_r.at[10], (m, lax.rem(r + k, ROW), c)).start()

    def squares_met():
        @pl.when(s == LAST)
        def _():
            arrived(sqz.at[pl.ds(0, COL - 1)], one_r.at[2])

        total = jnp.sum(sqz[...], axis=0)
        sqm[...] = total
        sqx[r] = total
        for k in range(1, ROW):
            remote(sqm, sqx.at[r], one_s.at[3], one_r.at[3], (s, lax.rem(r + k, ROW), c)).start()

    def roots():
        arrived(sqx.at[pl.ds(0, ROW - 1)], one_r.at[3])
        root = lax.rsqrt(jnp.sum(sqx[...], axis=0) / D + eps)
        for m in range(MB):
            rstd[m] = root[m : m + 1]

    stages = {"H": hidden, "V": halved, "S": summed, "P": spread, "F": features, "U": updated}
    for step, m in ORDER:
        if step == "q":
            squares_met()
        elif step == "r":
            roots()
        elif step == "g":
            arrived(gx.at[pl.ds(0, COL - 1)], one_r.at[1])
        else:
            stages[step](m)
        if step == "V" and m:

            @pl.when(s == LAST)
            def _(m=m - 1):
                slopes(m)

    @pl.when(s == LAST)
    def _():
        leanings()

    @pl.when(s != 0)
    def _():
        arrived(home, one_r.at[4])

    rough = home[...] + inc_t[...] - cot_t[...]
    part = jnp.concatenate([jnp.sum(v_t[i] * rough, axis=0, keepdims=True) for i in range(UPD)], axis=0)
    dxs[...] = part
    dxr[r] = part
    for k in range(1, ROW):
        remote(dxs, dxr.at[r], one_s.at[5], one_r.at[5], (s, lax.rem(r + k, ROW), c)).start()
    arrived(dxr.at[pl.ds(0, ROW - 1)], one_r.at[5])
    part = jnp.sum(dxr[...], axis=0)
    dzs[...] = part
    dzr[c] = part
    for k in FAR_Z:
        remote(dzs, dzr.at[c], one_s.at[6], one_r.at[6], (s, r, at_col(k))).start()

    @pl.when(s != 0)
    def _():
        arrived(khome, one_r.at[10])

    @pl.when(s == 0)
    def _():
        arrived(khome.at[pl.ds(0, ROW - 1)], one_r.at[10])

    k_all = jnp.sum(khome[...], axis=0)
    resid = home[...] - k_all * below[...].astype(f32) + inc_t[...] - cot_t[...]
    res_o[...] = resid
    tilt = k_all * jnp.sum(vzr[...], axis=0)
    arrived(dzr.at[pl.ds(0, COL - 1)], one_r.at[6])
    dots = jnp.sum(jnp.sum(dzr[...], axis=0) - tilt, axis=1, keepdims=True)
    update = dots[0:1] * u_t[0]
    for i in range(1, UPD):
        update = update + dots[i : i + 1] * u_t[i]
    new_o[...] = cot_t[...] + resid - update

    @pl.when(s == LAST)
    def _():
        left(gy.at[0, pl.ds(0, COL - 1)], first.at[0])

    @pl.when(s != LAST)
    def _():
        left(gy.at[0], first.at[0])
        left(cot_t, first.at[1])
        left(above_all.at[pl.ds(0, COL - 1)], one_s.at[9])

    @pl.when(s != 0)
    def _():
        left(x_v, one_s.at[7])

    @pl.when(s == 0)
    def _():
        left(x_v.at[pl.ds(1, MB - 1)], one_s.at[8])

    left(gx.at[pl.ds(0, COL - 1)], one_s.at[1])
    left(sqz.at[pl.ds(0, COL - 1)], one_s.at[2])
    left(sqx.at[pl.ds(0, ROW - 1)], one_s.at[3])
    left(vxr.at[pl.ds(0, ROW - 1)], one_s.at[11])
    left(vzr.at[pl.ds(0, COL - 1)], one_s.at[12])
    left(dxr.at[pl.ds(0, ROW - 1)], one_s.at[5])
    left(dzr.at[pl.ds(0, COL - 1)], one_s.at[6])

    def drained(m, carry_):
        @pl.when(s != 0)
        def _():
            left(gy.at[m], ss.at[0, m])

        @pl.when(jnp.logical_or(s != 0, m != 0))
        def _():
            left(after.at[m], ss.at[1, m])
            left(kpr.at[m], ss.at[7, m])

        @pl.when(jnp.logical_and(s == 0, m == 0))
        def _():
            left(kpr.at[m, pl.ds(0, ROW - 1)], ss.at[7, m])

        left(d1s.at[m], ss.at[2, m])
        left(xrv.at[m, pl.ds(0, XS - 1)], ss.at[3, m])
        left(ga.at[m, core, pl.ds(0, XS - 1)], ss.at[4, m])
        left(ga.at[m, core], ss.at[5, m])
        left(zr.at[m, pl.ds(0, COL - 1)], ss.at[6, m])
        left(kzr.at[m, pl.ds(0, COL - 1)], ss.at[8, m])
        return carry_

    lax.fori_loop(0, MB, drained, 0)


def turned(a):
    return jnp.swapaxes(a, -1, -2)


def shards(cotangent, incoming, upd_u, upd_v, saved_x, saved_h, norm_gain, w_gate, w_up, w_down):
    vm = pltpu.VMEM
    dma = pltpu.SemaphoreType.DMA
    tile = (CHUNK, ROWS)
    new, res = pl.pallas_call(
        kernel,
        out_shape=[jax.ShapeDtypeStruct(tile, f32)] * 2,
        in_specs=[pl.BlockSpec(memory_space=pl.ANY)] * 10,
        out_specs=[pl.BlockSpec(memory_space=pltpu.VMEM)] * 2,
        scratch_shapes=[
            vm(tile, f32),
            vm(tile, f32),
            vm((UPD, *tile), f32),
            vm((UPD, *tile), f32),
            vm((MB, *tile), bf16),
            vm((MB, 2, ROWS, HID), bf16),
            vm((1, CHUNK), f32),
            vm((2, FEATS, HALF), bf16),
            vm((2, FEATS, HALF), bf16),
            vm((ROW, PIECE, FEATS), bf16),
            vm((MB, *tile), f32),
            vm(tile, f32),
            vm((COL, MB, *tile), bf16),
            vm((MB, 2, 2, HALF, ROWS), f32),
            vm(tile, bf16),
            vm((MB, COL, *tile), bf16),
            vm((MB, *tile), bf16),
            vm((MB, *tile), f32),
            vm((MB, *tile), f32),
            vm((MB, XS, PIECE, ROWS), bf16),
            vm((MB, XS, PIECE, ROWS), bf16),
            vm((MB, XS, PIECE, ROWS), f32),
            vm((MB, XS, PIECE, ROWS), bf16),
            vm((MB, XS, PIECE, ROWS), bf16),
            vm((MB, PIECE, ROWS), f32),
            vm((MB, 2, XS, PIECE, ROWS), bf16),
            vm((2, HALF, ROWS), bf16),
            vm((FEATS, ROWS), f32),
            vm((MB, COL, *tile), bf16),
            vm((MB, COL, *tile), bf16),
            vm((MB, 1, ROWS), f32),
            vm((MB, COL, 1, ROWS), f32),
            vm((MB, 1, ROWS), f32),
            vm((MB, ROW, 1, ROWS), f32),
            vm((MB, *tile), bf16),
            vm((COL, MB, *tile), bf16),
            vm((MB, ROW, PIECE, ROWS), f32),
            vm(tile, bf16),
            vm((8, ROWS), f32),
            vm((COL, 8, ROWS), f32),
            vm((8, ROWS), f32),
            vm((ROW, 8, ROWS), f32),
            vm((MB, 1, ROWS), f32),
            vm(tile, f32),
            vm((ROW, 1, ROWS), f32),
            vm((UPD, ROWS), f32),
            vm((ROW, UPD, ROWS), f32),
            vm((UPD, ROWS), f32),
            vm((COL, UPD, ROWS), f32),
            vm((UPD, ROWS), f32),
            vm((ROW, UPD, ROWS), f32),
            vm((UPD, ROWS), f32),
            vm((COL, UPD, ROWS), f32),
            dma((12,)),
            dma((2,)),
            dma((9, MB)),
            dma((9, MB)),
            dma((13,)),
            dma((13,)),
        ],
        compiler_params=pltpu.CompilerParams(
            collective_id=0, has_side_effects=True, vmem_limit_bytes=60 * 1024 * 1024
        ),
        name="broyden",
    )(
        turned(cotangent), turned(incoming), turned(upd_u), turned(upd_v), turned(saved_x), saved_h, norm_gain,
        w_gate, w_up, w_down.reshape(1, ROW, PIECE, FEATS),
    )
    return new.T[None], res.T[None]


def solution(mesh):
    placed = (
        P("section", None, ("row", "col")),
        P("section", None, ("row", "col")),
        P("section", None, None, ("row", "col")),
        P("section", None, None, ("row", "col")),
        P("section", None, None, ("row", "col")),
        P("section", None, None, None, "col"),
        P("section", ("row", "col")),
        P("section", "row", "col"),
        P("section", "row", "col"),
        P("section", "col", "row"),
    )
    return jax.shard_map(
        shards,
        mesh=mesh,
        in_specs=placed,
        out_specs=(P("section", None, ("row", "col")), P("section", None, ("row", "col"))),
        check_vma=False,
    )
```

```python
import jax
import jax.numpy as jnp
from jax import lax
from jax.experimental import pallas as pl
from jax.experimental.pallas import tpu as pltpu
from jax.sharding import PartitionSpec as P

D = 4096
FF = 14336
ROWS = 128
UPD = 8
MB = 4
SECTIONS, ROW, COL = 4, 8, 8
XS = ROW // 2
CHUNK = D // (ROW * COL)
FEATS = D // ROW
HID = FF // COL
HALF = HID // 2
PIECE = HID // ROW
FAR_Z = (4, 3, 5, 2, 6, 1, 7)
FAR_X = (2, 1, 3)
FIRST_ORDER = [
    ("H", 3), ("V", 3), ("S", 3), ("H", 2), ("V", 2), ("q", 0), ("P", 3), ("g", 0), ("F", 3), ("S", 2),
    ("H", 1), ("V", 1), ("r", 0), ("U", 3), ("P", 2), ("F", 2), ("S", 1), ("H", 0), ("V", 0), ("U", 2),
    ("P", 1), ("F", 1), ("S", 0), ("U", 1), ("P", 0), ("F", 0), ("U", 0),
]
ORDER = [
    ("H", 3), ("V", 3), ("S", 3), ("H", 2), ("V", 2), ("q", 0), ("P", 3), ("g", 0), ("F", 3), ("S", 2),
    ("H", 1), ("V", 1), ("r", 0), ("U", 3), ("P", 2), ("F", 2), ("S", 1), ("H", 0), ("V", 0), ("U", 2),
    ("P", 1), ("F", 1), ("S", 0), ("U", 1), ("P", 0), ("F", 0), ("e", 0), ("d", 0), ("U", 0),
]

eps = 1e-05
bf16 = jnp.bfloat16
f32 = jnp.float32
MESH = pl.DeviceIdType.MESH


def kernel(
    cot_h, inc_h, u_h, v_h, x_h, h_h, gain_h, wg_h, wu_h, wd_h,
    new_o, res_o,
    cot_t, inc_t, u_t, v_t, x_v, h_v, gain_v, wg_v, wu_v, wd_v,
    x_t, gain_t, gx, gv, slope,
    start, gy, gys, carry, after, d1s, d1r, own, xsd, xrv, mine, ga, grads, acc, zs, zr,
    kzs, kzr, kps, kpr, above, above_all, lean, below, sqs, sqz, sqm, sqx, rstd, home, khome, kall, vxs, vxr, vzs, vzr, dxs, dxr, dzs, dzr,
    load, first, ss, rs, one_s, one_r,
):
    s = lax.axis_index("section")
    r = lax.axis_index("row")
    c = lax.axis_index("col")
    core = lax.rem(r, 2)
    x = lax.div(r, 2)
    mate = r + 1 - 2 * core

    def at_col(k):
        return lax.rem(c + k, COL)

    def at_x(k):
        return lax.rem(x + k, XS)

    def remote(src, dst, send, recv, device):
        return pltpu.make_async_remote_copy(
            src_ref=src, dst_ref=dst, send_sem=send, recv_sem=recv, device_id=device, device_id_type=MESH
        )

    def arrived(ref, recv):
        remote(ref, ref, one_s.at[0], recv, (s, mate, c)).wait_recv()

    def left(ref, send):
        remote(ref, ref, send, one_r.at[0], (s, mate, c)).wait_send()

    barrier = pltpu.get_barrier_semaphore()
    for k in FAR_Z:
        pl.semaphore_signal(barrier, inc=1, device_id=(s, r, at_col(k)), device_id_type=MESH)
    for k in (2, 1, 3):
        pl.semaphore_signal(barrier, inc=1, device_id=(lax.rem(s + k, SECTIONS), r, c), device_id_type=MESH)
    for k in range(1, ROW):
        pl.semaphore_signal(barrier, inc=1, device_id=(s, lax.rem(r + k, ROW), c), device_id_type=MESH)

    loads = {}
    for i, (name, src, dst) in enumerate(
        (
            ("cot", cot_h.at[0], cot_t),
            ("gain", gain_h, gain_v),
            ("x", x_h.at[0], x_v),
            ("wd", wd_h.at[0], wd_v),
            ("h", h_h.at[0], h_v),
            ("wg0", wg_h.at[0, :, pl.ds(0, HALF)], wg_v.at[0]),
            ("wg1", wg_h.at[0, :, pl.ds(HALF, HALF)], wg_v.at[1]),
            ("wu0", wu_h.at[0, :, pl.ds(0, HALF)], wu_v.at[0]),
            ("wu1", wu_h.at[0, :, pl.ds(HALF, HALF)], wu_v.at[1]),
            ("inc", inc_h.at[0], inc_t),
            ("u", u_h.at[0], u_t),
            ("v", v_h.at[0], v_t),
        )
    ):
        loads[name] = pltpu.make_async_copy(src, dst, load.at[i])
        loads[name].start()

    loads["cot"].wait()
    start[...] = cot_t[...].astype(bf16)
    pl.semaphore_wait(barrier, SECTIONS - 1 + COL - 1 + ROW - 1)

    LAST = SECTIONS - 1
    mb_home = s

    @pl.when(s == LAST)
    def _():
        gy[LAST, c] = start[...]
        carry[LAST] = cot_t[...]
        for k in FAR_Z:
            remote(
                start, gy.at[LAST, c], first.at[0], rs.at[0, LAST], (LAST, r, at_col(k))
            ).start()

    loads["x"].wait()

    @pl.when(s != 0)
    def _():
        remote(x_v, above, one_s.at[7], one_r.at[7], (s - 1, r, c)).start()

    @pl.when(s == 0)
    def _():
        for m in range(1, MB):
            remote(x_v.at[m], below, one_s.at[8], one_r.at[8], (m, r, c)).start()
        below[...] = x_v[0]

    loads["gain"].wait()
    gain_t[...] = jnp.broadcast_to(gain_v[...], (ROWS, CHUNK)).T
    sums = []
    for m in range(MB):
        xt = x_v[m].astype(f32)
        x_t[m] = xt
        gx[c, m] = (gain_t[...] * xt).astype(bf16)
        sums.append(jnp.sum(xt * xt, axis=0, keepdims=True))
    sums = jnp.concatenate(sums + sums, axis=0)
    sqs[...] = sums
    sqz[c] = sums
    for k in FAR_Z:
        remote(sqs, sqz.at[c], one_s.at[2], one_r.at[2], (s, r, at_col(k))).start()

    @pl.when(s != LAST)
    def _():
        arrived(sqz.at[pl.ds(0, COL - 1)], one_r.at[2])
        for k in (*FAR_Z, 0):
            remote(start, gy.at[mb_home, c], first.at[0], rs.at[0, mb_home], (LAST, r, at_col(k))).start()
        remote(cot_t, carry.at[mb_home], first.at[1], rs.at[1, mb_home], (LAST, r, c)).start()
        arrived(above, one_r.at[7])
        above_all[c] = above[...]
        for k in FAR_Z:
            remote(above, above_all.at[c], one_s.at[9], one_r.at[9], (s, r, at_col(k))).start()

    for k in FAR_Z:
        remote(gx.at[c], gx.at[c], one_s.at[1], one_r.at[1], (s, r, at_col(k))).start()

    def slopes(m):
        for half in range(2):
            for b in range(7):
                at = pl.ds(half * HALF + b * 128, 128)
                hg = h_v[m, 0, :, at].astype(f32)
                hu = h_v[m, 1, :, at].astype(f32)
                sig = jax.nn.sigmoid(hg)
                slope[m, 0, half, pl.ds(b * 128, 128)] = (hu * sig * (1.0 + hg * (1.0 - sig))).T
                slope[m, 1, half, pl.ds(b * 128, 128)] = (hg * sig).T

    loads["h"].wait()
    loads["inc"].wait()
    loads["u"].wait()
    loads["v"].wait()

    @pl.when(s != LAST)
    def _():
        def body(m, carry_):
            slopes(m)
            return carry_

        lax.fori_loop(0, MB, body, 0)

    @pl.when(s == LAST)
    def _():
        slopes(LAST)

    for name in ("wd", "wg0", "wg1", "wu0", "wu1"):
        loads[name].wait()

    def leanings():
        @pl.when(s != 0)
        def _():
            arrived(below, one_r.at[8])

        b = below[...].astype(f32)
        part = jnp.concatenate([jnp.sum(v_t[i] * b, axis=0, keepdims=True) for i in range(UPD)], axis=0)
        vxs[...] = part
        vxr[r] = part
        for k in range(1, ROW):
            remote(vxs, vxr.at[r], one_s.at[11], one_r.at[11], (s, lax.rem(r + k, ROW), c)).start()
        arrived(vxr.at[pl.ds(0, ROW - 1)], one_r.at[11])
        part = jnp.sum(vxr[...], axis=0)
        vzs[...] = part
        vzr[c] = part
        for k in FAR_Z:
            remote(vzs, vzr.at[c], one_s.at[12], one_r.at[12], (s, r, at_col(k))).start()
        arrived(vzr.at[pl.ds(0, COL - 1)], one_r.at[12])

    @pl.when(s != LAST)
    def _():
        leanings()

    @pl.when(s == 0)
    def _():
        for i in range(UPD):
            gv[c, i] = (gain_t[...] * v_t[i]).astype(bf16)
        for k in FAR_Z:
            remote(gv.at[c], gv.at[c], one_s.at[13], one_r.at[13], (s, r, at_col(k))).start()

    @pl.when(s != LAST)
    def _():
        arrived(above_all.at[pl.ds(0, COL - 1)], one_r.at[9])

        def body(m, carry_):
            a = above_all[:, m].reshape(FEATS, ROWS)
            for i in range(ROW):
                lean[m, i] = jnp.dot(wd_v[i], a, preferred_element_type=f32)
            return carry_

        lax.fori_loop(0, MB, body, 0)

    @pl.when(s == 0)
    def _():
        arrived(gv.at[pl.ds(0, COL - 1)], one_r.at[13])

    def hidden(m, first):
        if first and m == LAST:
            arrived(gy.at[m, pl.ds(0, COL - 1)], rs.at[0, m])
        else:
            arrived(gy.at[m], rs.at[0, m])
            arrived(carry.at[m], rs.at[1, m])
        if not first:
            arrived(kpr.at[m], rs.at[7, m])
            k = jnp.sum(kpr[m], axis=0)
        g = gy[m].reshape(FEATS, ROWS)

        def product(q):
            whole = jnp.dot(wd_v[q], g, preferred_element_type=f32)
            return whole if first else whole - k * lean[m, q]

        for i in range(XS):
            d1s[m, i] = product((1 - core) * XS + i).astype(bf16)
        remote(d1s.at[m], d1r.at[m], ss.at[2, m], rs.at[2, m], (s, mate, c)).start()
        for i in range(XS):
            own[m, i] = product(core * XS + i)
        if not first:
            carry[m] = carry[m] - k * above[m].astype(f32)

    def halved(m):
        arrived(d1r.at[m], rs.at[2, m])
        for k in FAR_X:
            to = at_x(k)
            xsd[m, to] = (own[m, to] + d1r[m, to].astype(f32)).astype(bf16)
            remote(xsd.at[m, to], xrv.at[m, x], ss.at[3, m], rs.at[3, m], (s, 2 * to + core, c)).start()
        mine[m] = own[m, x] + d1r[m, x].astype(f32)

    def summed(m):
        arrived(xrv.at[m, pl.ds(0, XS - 1)], rs.at[3, m])
        total = mine[m]
        for k in FAR_X:
            total = total + xrv[m, at_x(k)].astype(f32)
        ga[m, core, x] = total.astype(bf16)
        for k in FAR_X:
            remote(ga.at[m, core, x], ga.at[m, core, x], ss.at[4, m], rs.at[4, m], (s, 2 * at_x(k) + core, c)).start()

    def gradients(m, half):
        g = ga[m, half].reshape(HALF, ROWS).astype(f32)
        grads[0] = (g * slope[m, 0, half]).astype(bf16)
        grads[1] = (g * slope[m, 1, half]).astype(bf16)

    def spread(m):
        arrived(ga.at[m, core, pl.ds(0, XS - 1)], rs.at[4, m])
        remote(ga.at[m, core], ga.at[m, core], ss.at[5, m], rs.at[5, m], (s, mate, c)).start()
        gradients(m, core)
        for b in range(2):
            rows = pl.ds(b * 256, 256)
            acc[rows] = jnp.dot(wg_v[core, rows], grads[0], preferred_element_type=f32) + jnp.dot(
                wu_v[core, rows], grads[1], preferred_element_type=f32
            )

    def features(m):
        other = 1 - core
        arrived(ga.at[m, other], rs.at[5, m])
        gradients(m, other)
        inner = jnp.zeros((1, ROWS), f32)
        for b in range(2):
            rows = pl.ds(b * 256, 256)
            part = (
                acc[rows]
                + jnp.dot(wg_v[other, rows], grads[0], preferred_element_type=f32)
                + jnp.dot(wu_v[other, rows], grads[1], preferred_element_type=f32)
            )
            scaled = gx[pl.ds(4 * b, 4), m].reshape(256, ROWS).astype(f32)
            inner = inner + jnp.sum(part * scaled, axis=0, keepdims=True)
            zs[m, pl.ds(4 * b, 4)] = part.astype(bf16).reshape(4, CHUNK, ROWS)
            if m == 0:
                acc[rows] = part
        for k in FAR_Z:
            to = at_col(k)
            remote(zs.at[m, to], zr.at[m, c], ss.at[6, m], rs.at[6, m], (s, r, to)).start()
        kzs[m] = inner
        for k in FAR_Z:
            remote(kzs.at[m], kzr.at[m, c], ss.at[8, m], rs.at[8, m], (s, r, at_col(k))).start()
        zr[m, c] = zs[m, c]
        kzr[m, c] = inner

    def early():
        known = carry[0] + inc_t[...] - cot_t[...]
        found = []
        for i in range(UPD):
            total = jnp.zeros((1, ROWS), f32)
            for b in range(2):
                scaled = gv[pl.ds(4 * b, 4), i].reshape(256, ROWS).astype(f32)
                total = total + jnp.sum(acc[pl.ds(b * 256, 256)] * scaled, axis=0, keepdims=True)
            found.append(rstd[0] * total + jnp.sum(v_t[i] * known, axis=0, keepdims=True))
        meet_row(jnp.concatenate([*found, kzs[0], jnp.zeros((7, ROWS), f32)], axis=0))

    def meet_row(part):
        dxs[...] = part
        dxr[r] = part
        for k in range(1, ROW):
            remote(dxs, dxr.at[r], one_s.at[5], one_r.at[5], (s, lax.rem(r + k, ROW), c)).start()

    def meet_col():
        arrived(dxr.at[pl.ds(0, ROW - 1)], one_r.at[5])
        part = jnp.sum(dxr[...], axis=0)
        dzs[...] = part
        dzr[c] = part
        for k in FAR_Z:
            remote(dzs, dzr.at[c], one_s.at[6], one_r.at[6], (s, r, at_col(k))).start()

    def updated(m):
        arrived(zr.at[m, pl.ds(0, COL - 1)], rs.at[6, m])
        arrived(kzr.at[m, pl.ds(0, COL - 1)], rs.at[8, m])
        total = jnp.sum(zr[m].astype(f32), axis=0)
        inner = jnp.sum(kzr[m], axis=0)
        root = rstd[m]
        fresh = carry[m] + root * (gain_t[...] * total)
        after[m] = fresh
        kps[m] = (root * root * root) * (inner / D)

        @pl.when(s != 0)
        def _():
            gys[m] = fresh.astype(bf16)
            for k in (*FAR_Z, 0):
                remote(
                    gys.at[m], gy.at[m, c], ss.at[0, m], rs.at[0, m], (s - 1, r, at_col(k))
                ).start()
            for k in range(ROW):
                remote(kps.at[m], kpr.at[m, r], ss.at[7, m], rs.at[7, m], (s - 1, lax.rem(r + k, ROW), c)).start()
            remote(after.at[m], carry.at[m], ss.at[1, m], rs.at[1, m], (s - 1, r, c)).start()

        @pl.when(s == 0)
        def _():
            if m == 0:
                home[...] = fresh
            else:
                remote(after.at[m], home, ss.at[1, m], one_r.at[4], (m, r, c)).start()
                for k in range(ROW):
                    remote(kps.at[m], khome.at[r], ss.at[7, m], one_r.at[10], (m, lax.rem(r + k, ROW), c)).start()

    def squares_met():
        total = jnp.sum(sqz[...], axis=0)
        sqm[...] = total
        sqx[r] = total
        for k in range(1, ROW):
            remote(sqm, sqx.at[r], one_s.at[3], one_r.at[3], (s, lax.rem(r + k, ROW), c)).start()

    def roots():
        arrived(sqx.at[pl.ds(0, ROW - 1)], one_r.at[3])
        root = lax.rsqrt(jnp.sum(sqx[...], axis=0) / D + eps)
        for m in range(MB):
            rstd[m] = root[m : m + 1]

    stages = {"V": halved, "S": summed, "P": spread, "F": features, "U": updated}

    def play(order, first):
        for step, m in order:
            if step == "H":
                hidden(m, first)
            elif step == "q":
                if first:
                    arrived(sqz.at[pl.ds(0, COL - 1)], one_r.at[2])
                squares_met()
            elif step == "r":
                roots()
            elif step == "g":
                arrived(gx.at[pl.ds(0, COL - 1)], one_r.at[1])
            elif step == "e":

                @pl.when(s == 0)
                def _():
                    early()

            elif step == "d":

                @pl.when(s == 0)
                def _():
                    meet_col()

            else:
                stages[step](m)
            if step == "V" and m and first:
                slopes(m - 1)

    @pl.when(s == LAST)
    def _():
        play(FIRST_ORDER, True)

    @pl.when(s != LAST)
    def _():
        play(ORDER, False)

    @pl.when(s == LAST)
    def _():
        leanings()

    @pl.when(s != 0)
    def _():
        arrived(home, one_r.at[4])
        rough = home[...] + inc_t[...] - cot_t[...]
        part = [jnp.sum(v_t[i] * rough, axis=0, keepdims=True) for i in range(UPD)]
        meet_row(jnp.concatenate([*part, jnp.zeros((8, ROWS), f32)], axis=0))
        meet_col()
        arrived(khome, one_r.at[10])
        kall[...] = jnp.sum(khome[...], axis=0)

    arrived(dzr.at[pl.ds(0, COL - 1)], one_r.at[6])
    met = jnp.sum(dzr[...], axis=0)

    @pl.when(s == 0)
    def _():
        kall[...] = (rstd[0] * rstd[0] * rstd[0]) * (met[UPD : UPD + 1] / D)

    resid = home[...] - kall[...] * below[...].astype(f32) + inc_t[...] - cot_t[...]
    res_o[...] = resid
    dots = jnp.sum(met[:UPD] - kall[...] * jnp.sum(vzr[...], axis=0), axis=1, keepdims=True)
    update = dots[0:1] * u_t[0]
    for i in range(1, UPD):
        update = update + dots[i : i + 1] * u_t[i]
    new_o[...] = cot_t[...] + resid - update

    @pl.when(s == LAST)
    def _():
        left(gy.at[0, pl.ds(0, COL - 1)], first.at[0])

    @pl.when(s != LAST)
    def _():
        left(gy.at[0], first.at[0])
        left(cot_t, first.at[1])
        left(above_all.at[pl.ds(0, COL - 1)], one_s.at[9])

    @pl.when(s != 0)
    def _():
        left(x_v, one_s.at[7])

    @pl.when(s == 0)
    def _():
        left(gv.at[pl.ds(0, COL - 1)], one_s.at[13])
        left(x_v.at[pl.ds(1, MB - 1)], one_s.at[8])

    left(gx.at[pl.ds(0, COL - 1)], one_s.at[1])
    left(sqz.at[pl.ds(0, COL - 1)], one_s.at[2])
    left(sqx.at[pl.ds(0, ROW - 1)], one_s.at[3])
    left(vxr.at[pl.ds(0, ROW - 1)], one_s.at[11])
    left(vzr.at[pl.ds(0, COL - 1)], one_s.at[12])
    left(dxr.at[pl.ds(0, ROW - 1)], one_s.at[5])
    left(dzr.at[pl.ds(0, COL - 1)], one_s.at[6])

    def drained(m, carry_):
        @pl.when(s != 0)
        def _():
            left(gy.at[m], ss.at[0, m])

        @pl.when(jnp.logical_or(s != 0, m != 0))
        def _():
            left(after.at[m], ss.at[1, m])
            left(kpr.at[m], ss.at[7, m])

        left(d1s.at[m], ss.at[2, m])
        left(xrv.at[m, pl.ds(0, XS - 1)], ss.at[3, m])
        left(ga.at[m, core, pl.ds(0, XS - 1)], ss.at[4, m])
        left(ga.at[m, core], ss.at[5, m])
        left(zr.at[m, pl.ds(0, COL - 1)], ss.at[6, m])
        left(kzr.at[m, pl.ds(0, COL - 1)], ss.at[8, m])
        return carry_

    lax.fori_loop(0, MB, drained, 0)


def turned(a):
    return jnp.swapaxes(a, -1, -2)


def shards(cotangent, incoming, upd_u, upd_v, saved_x, saved_h, norm_gain, w_gate, w_up, w_down):
    vm = pltpu.VMEM
    dma = pltpu.SemaphoreType.DMA
    tile = (CHUNK, ROWS)
    new, res = pl.pallas_call(
        kernel,
        out_shape=[jax.ShapeDtypeStruct(tile, f32)] * 2,
        in_specs=[pl.BlockSpec(memory_space=pl.ANY)] * 10,
        out_specs=[pl.BlockSpec(memory_space=pltpu.VMEM)] * 2,
        scratch_shapes=[
            vm(tile, f32),
            vm(tile, f32),
            vm((UPD, *tile), f32),
            vm((UPD, *tile), f32),
            vm((MB, *tile), bf16),
            vm((MB, 2, ROWS, HID), bf16),
            vm((1, CHUNK), f32),
            vm((2, FEATS, HALF), bf16),
            vm((2, FEATS, HALF), bf16),
            vm((ROW, PIECE, FEATS), bf16),
            vm((MB, *tile), f32),
            vm(tile, f32),
            vm((COL, MB, *tile), bf16),
            vm((COL, UPD, *tile), bf16),
            vm((MB, 2, 2, HALF, ROWS), f32),
            vm(tile, bf16),
            vm((MB, COL, *tile), bf16),
            vm((MB, *tile), bf16),
            vm((MB, *tile), f32),
            vm((MB, *tile), f32),
            vm((MB, XS, PIECE, ROWS), bf16),
            vm((MB, XS, PIECE, ROWS), bf16),
            vm((MB, XS, PIECE, ROWS), f32),
            vm((MB, XS, PIECE, ROWS), bf16),
            vm((MB, XS, PIECE, ROWS), bf16),
            vm((MB, PIECE, ROWS), f32),
            vm((MB, 2, XS, PIECE, ROWS), bf16),
            vm((2, HALF, ROWS), bf16),
            vm((FEATS, ROWS), f32),
            vm((MB, COL, *tile), bf16),
            vm((MB, COL, *tile), bf16),
            vm((MB, 1, ROWS), f32),
            vm((MB, COL, 1, ROWS), f32),
            vm((MB, 1, ROWS), f32),
            vm((MB, ROW, 1, ROWS), f32),
            vm((MB, *tile), bf16),
            vm((COL, MB, *tile), bf16),
            vm((MB, ROW, PIECE, ROWS), f32),
            vm(tile, bf16),
            vm((8, ROWS), f32),
            vm((COL, 8, ROWS), f32),
            vm((8, ROWS), f32),
            vm((ROW, 8, ROWS), f32),
            vm((MB, 1, ROWS), f32),
            vm(tile, f32),
            vm((ROW, 1, ROWS), f32),
            vm((1, ROWS), f32),
            vm((UPD, ROWS), f32),
            vm((ROW, UPD, ROWS), f32),
            vm((UPD, ROWS), f32),
            vm((COL, UPD, ROWS), f32),
            vm((2 * UPD, ROWS), f32),
            vm((ROW, 2 * UPD, ROWS), f32),
            vm((2 * UPD, ROWS), f32),
            vm((COL, 2 * UPD, ROWS), f32),
            dma((12,)),
            dma((2,)),
            dma((9, MB)),
            dma((9, MB)),
            dma((14,)),
            dma((14,)),
        ],
        compiler_params=pltpu.CompilerParams(
            collective_id=0, has_side_effects=True, vmem_limit_bytes=60 * 1024 * 1024
        ),
        name="broyden",
    )(
        turned(cotangent), turned(incoming), turned(upd_u), turned(upd_v), turned(saved_x), saved_h, norm_gain,
        w_gate, w_up, w_down.reshape(1, ROW, PIECE, FEATS),
    )
    return new.T[None], res.T[None]


def solution(mesh):
    placed = (
        P("section", None, ("row", "col")),
        P("section", None, ("row", "col")),
        P("section", None, None, ("row", "col")),
        P("section", None, None, ("row", "col")),
        P("section", None, None, ("row", "col")),
        P("section", None, None, None, "col"),
        P("section", ("row", "col")),
        P("section", "row", "col"),
        P("section", "row", "col"),
        P("section", "col", "row"),
    )
    return jax.shard_map(
        shards,
        mesh=mesh,
        in_specs=placed,
        out_specs=(P("section", None, ("row", "col")), P("section", None, ("row", "col"))),
        check_vma=False,
    )
```

```python
import jax
import jax.numpy as jnp
from jax import lax
from jax.experimental import pallas as pl
from jax.experimental.pallas import tpu as pltpu
from jax.sharding import PartitionSpec as P

D = 4096
FF = 14336
ROWS = 128
UPD = 8
MB = 4
SECTIONS, ROW, COL = 4, 8, 8
XS = ROW // 2
CHUNK = D // (ROW * COL)
FEATS = D // ROW
HID = FF // COL
HALF = HID // 2
PIECE = HID // ROW
PARTS = 2
PART = PIECE // PARTS
FAR_Z = (4, 3, 5, 2, 6, 1, 7)
FAR_X = (2, 1, 3)
FIRST_ORDER = [
    ("H", 3), ("V", 3), ("S", 3), ("H", 2), ("V", 2), ("q", 0), ("P", 3), ("g", 0), ("F", 3), ("S", 2),
    ("H", 1), ("V", 1), ("r", 0), ("U", 3), ("P", 2), ("F", 2), ("S", 1), ("H", 0), ("V", 0), ("U", 2),
    ("P", 1), ("F", 1), ("S", 0), ("U", 1), ("P", 0), ("F", 0), ("U", 0),
]
ORDER = [
    ("H", 3), ("V", 3), ("S", 3), ("H", 2), ("V", 2), ("q", 0), ("P", 3), ("g", 0), ("F", 3), ("S", 2),
    ("H", 1), ("V", 1), ("r", 0), ("U", 3), ("P", 2), ("F", 2), ("S", 1), ("H", 0), ("V", 0), ("U", 2),
    ("P", 1), ("F", 1), ("S", 0), ("U", 1), ("P", 0), ("F", 0), ("e", 0), ("d", 0), ("U", 0),
]

eps = 1e-05
bf16 = jnp.bfloat16
f32 = jnp.float32
MESH = pl.DeviceIdType.MESH


def kernel(
    cot_h, inc_h, u_h, v_h, x_h, h_h, gain_h, wg_h, wu_h, wd_h,
    out_o,
    cot_t, inc_t, u_t, v_t, x_v, h_v, gain_v, wg_v, wu_v, wd_v,
    x_t, gain_t, gx, gv, slope,
    start, gy, gys, carry, after, d1s, d1r, own, xsd, xrv, mine, ga, grads, acc, zs, zr,
    kzs, kzr, kps, kpr, above, above_all, lean, below, sqs, sqz, sqm, sqx, rstd, home, khome, kall, vxs, vxr, vzs, vzr, dxs, dxr, dzs, dzr,
    load, first, ss, rs, split, one_s, one_r,
):
    s = lax.axis_index("section")
    r = lax.axis_index("row")
    c = lax.axis_index("col")
    core = lax.rem(r, 2)
    x = lax.div(r, 2)
    mate = r + 1 - 2 * core

    def at_col(k):
        return lax.rem(c + k, COL)

    def at_x(k):
        return lax.rem(x + k, XS)

    def remote(src, dst, send, recv, device):
        return pltpu.make_async_remote_copy(
            src_ref=src, dst_ref=dst, send_sem=send, recv_sem=recv, device_id=device, device_id_type=MESH
        )

    def arrived(ref, recv):
        remote(ref, ref, one_s.at[0], recv, (s, mate, c)).wait_recv()

    def left(ref, send):
        remote(ref, ref, send, one_r.at[0], (s, mate, c)).wait_send()

    barrier = pltpu.get_barrier_semaphore()
    for k in FAR_Z:
        pl.semaphore_signal(barrier, inc=1, device_id=(s, r, at_col(k)), device_id_type=MESH)
    for k in (2, 1, 3):
        pl.semaphore_signal(barrier, inc=1, device_id=(lax.rem(s + k, SECTIONS), r, c), device_id_type=MESH)
    for k in range(1, ROW):
        pl.semaphore_signal(barrier, inc=1, device_id=(s, lax.rem(r + k, ROW), c), device_id_type=MESH)

    loads = {}
    for i, (name, src, dst) in enumerate(
        (
            ("cot", cot_h.at[0], cot_t),
            ("gain", gain_h, gain_v),
            ("x", x_h.at[0], x_v),
            ("wd", wd_h.at[0], wd_v),
            ("h", h_h.at[0], h_v),
            ("wg0", wg_h.at[0, :, pl.ds(0, HALF)], wg_v.at[0]),
            ("wg1", wg_h.at[0, :, pl.ds(HALF, HALF)], wg_v.at[1]),
            ("wu0", wu_h.at[0, :, pl.ds(0, HALF)], wu_v.at[0]),
            ("wu1", wu_h.at[0, :, pl.ds(HALF, HALF)], wu_v.at[1]),
            ("inc", inc_h.at[0], inc_t),
            ("u", u_h.at[0], u_t),
            ("v", v_h.at[0], v_t),
        )
    ):
        loads[name] = pltpu.make_async_copy(src, dst, load.at[i])
        loads[name].start()

    loads["cot"].wait()
    start[...] = cot_t[...].astype(bf16)
    pl.semaphore_wait(barrier, SECTIONS - 1 + COL - 1 + ROW - 1)

    LAST = SECTIONS - 1
    mb_home = s

    @pl.when(s == LAST)
    def _():
        gy[LAST, c] = start[...]
        carry[LAST] = cot_t[...]
        for k in FAR_Z:
            remote(
                start, gy.at[LAST, c], first.at[0], rs.at[0, LAST], (LAST, r, at_col(k))
            ).start()

    loads["x"].wait()

    @pl.when(s != 0)
    def _():
        remote(x_v, above, one_s.at[7], one_r.at[7], (s - 1, r, c)).start()

    @pl.when(s == 0)
    def _():
        for m in range(1, MB):
            remote(x_v.at[m], below, one_s.at[8], one_r.at[8], (m, r, c)).start()
        below[...] = x_v[0]

    loads["gain"].wait()
    gain_t[...] = jnp.broadcast_to(gain_v[...], (ROWS, CHUNK)).T
    sums = []
    for m in range(MB):
        xt = x_v[m].astype(f32)
        x_t[m] = xt
        gx[c, m] = (gain_t[...] * xt).astype(bf16)
        sums.append(jnp.sum(xt * xt, axis=0, keepdims=True))
    sums = jnp.concatenate(sums + sums, axis=0)
    sqs[...] = sums
    sqz[c] = sums
    for k in FAR_Z:
        remote(sqs, sqz.at[c], one_s.at[2], one_r.at[2], (s, r, at_col(k))).start()

    @pl.when(s != LAST)
    def _():
        arrived(sqz.at[pl.ds(0, COL - 1)], one_r.at[2])
        for k in (*FAR_Z, 0):
            remote(start, gy.at[mb_home, c], first.at[0], rs.at[0, mb_home], (LAST, r, at_col(k))).start()
        remote(cot_t, carry.at[mb_home], first.at[1], rs.at[1, mb_home], (LAST, r, c)).start()
        arrived(above, one_r.at[7])
        above_all[c] = above[...]
        for k in FAR_Z:
            remote(above, above_all.at[c], one_s.at[9], one_r.at[9], (s, r, at_col(k))).start()

    for k in FAR_Z:
        remote(gx.at[c], gx.at[c], one_s.at[1], one_r.at[1], (s, r, at_col(k))).start()

    def slopes(m):
        for half in range(2):
            for b in range(7):
                at = pl.ds(half * HALF + b * 128, 128)
                hg = h_v[m, 0, :, at].astype(f32)
                hu = h_v[m, 1, :, at].astype(f32)
                sig = jax.nn.sigmoid(hg)
                slope[m, 0, half, pl.ds(b * 128, 128)] = (hu * sig * (1.0 + hg * (1.0 - sig))).T
                slope[m, 1, half, pl.ds(b * 128, 128)] = (hg * sig).T

    loads["h"].wait()
    loads["inc"].wait()
    loads["u"].wait()
    loads["v"].wait()

    @pl.when(s != LAST)
    def _():
        def body(m, carry_):
            slopes(m)
            return carry_

        lax.fori_loop(0, MB, body, 0)

    @pl.when(s == LAST)
    def _():
        slopes(LAST)

    for name in ("wd", "wg0", "wg1", "wu0", "wu1"):
        loads[name].wait()

    def leanings():
        @pl.when(s != 0)
        def _():
            arrived(below, one_r.at[8])

        b = below[...].astype(f32)
        part = jnp.concatenate([jnp.sum(v_t[i] * b, axis=0, keepdims=True) for i in range(UPD)], axis=0)
        vxs[...] = part
        vxr[r] = part
        for k in range(1, ROW):
            remote(vxs, vxr.at[r], one_s.at[11], one_r.at[11], (s, lax.rem(r + k, ROW), c)).start()

    def leanings_met():
        arrived(vxr.at[pl.ds(0, ROW - 1)], one_r.at[11])
        part = jnp.sum(vxr[...], axis=0)
        vzs[...] = part
        vzr[c] = part
        for k in FAR_Z:
            remote(vzs, vzr.at[c], one_s.at[12], one_r.at[12], (s, r, at_col(k))).start()

    @pl.when(s != LAST)
    def _():
        leanings()

    @pl.when(s == 0)
    def _():
        for i in range(UPD):
            gv[c, i] = (gain_t[...] * v_t[i]).astype(bf16)
        for k in FAR_Z:
            remote(gv.at[c], gv.at[c], one_s.at[13], one_r.at[13], (s, r, at_col(k))).start()

    @pl.when(s != LAST)
    def _():
        arrived(above_all.at[pl.ds(0, COL - 1)], one_r.at[9])

        def body(m, carry_):
            a = above_all[:, m].reshape(FEATS, ROWS)
            for i in range(ROW):
                lean[m, i] = jnp.dot(wd_v[i], a, preferred_element_type=f32)
            return carry_

        lax.fori_loop(0, MB, body, 0)
        leanings_met()

    @pl.when(s == 0)
    def _():
        arrived(gv.at[pl.ds(0, COL - 1)], one_r.at[13])

    def hidden(m, first):
        if first and m == LAST:
            arrived(gy.at[m, pl.ds(0, COL - 1)], rs.at[0, m])
        else:
            arrived(gy.at[m], rs.at[0, m])
            arrived(carry.at[m], rs.at[1, m])
        if not first:
            arrived(kpr.at[m], rs.at[7, m])
            k = jnp.sum(kpr[m], axis=0)
        g = gy[m].reshape(FEATS, ROWS)

        def product(q, b):
            rows = pl.ds(b * PART, PART)
            whole = jnp.dot(wd_v[q, rows], g, preferred_element_type=f32)
            return whole if first else whole - k * lean[m, q, rows]

        for b in range(PARTS):
            for i in range(XS):
                d1s[m, b, i] = product((1 - core) * XS + i, b).astype(bf16)
            remote(d1s.at[m, b], d1r.at[m, b], ss.at[2, m], split.at[0, b, m], (s, mate, c)).start()
        for b in range(PARTS):
            for i in range(XS):
                own[m, b, i] = product(core * XS + i, b)
        if not first:
            carry[m] = carry[m] - k * above[m].astype(f32)

    def halved(m):
        for b in range(PARTS):
            arrived(d1r.at[m, b], split.at[0, b, m])
            for k in FAR_X:
                to = at_x(k)
                xsd[m, b, to] = (own[m, b, to] + d1r[m, b, to].astype(f32)).astype(bf16)
                remote(
                    xsd.at[m, b, to], xrv.at[m, b, x], ss.at[3, m], split.at[1, b, m], (s, 2 * to + core, c)
                ).start()
            mine[m, b] = own[m, b, x] + d1r[m, b, x].astype(f32)

    def summed(m):
        for b in range(PARTS):
            arrived(xrv.at[m, b, pl.ds(0, XS - 1)], split.at[1, b, m])
            total = mine[m, b]
            for k in FAR_X:
                total = total + xrv[m, b, at_x(k)].astype(f32)
            ga[m, core, x, b] = total.astype(bf16)
            for k in FAR_X:
                remote(
                    ga.at[m, core, x, b], ga.at[m, core, x, b], ss.at[4, m], rs.at[4, m], (s, 2 * at_x(k) + core, c)
                ).start()

    def gradients(m, half):
        g = ga[m, half].reshape(HALF, ROWS).astype(f32)
        grads[0] = (g * slope[m, 0, half]).astype(bf16)
        grads[1] = (g * slope[m, 1, half]).astype(bf16)

    def spread(m):
        arrived(ga.at[m, core, pl.ds(0, XS - 1)], rs.at[4, m])
        remote(ga.at[m, core], ga.at[m, core], ss.at[5, m], rs.at[5, m], (s, mate, c)).start()
        gradients(m, core)
        for b in range(2):
            rows = pl.ds(b * 256, 256)
            acc[rows] = jnp.dot(wg_v[core, rows], grads[0], preferred_element_type=f32) + jnp.dot(
                wu_v[core, rows], grads[1], preferred_element_type=f32
            )

    def features(m):
        other = 1 - core
        arrived(ga.at[m, other], rs.at[5, m])
        gradients(m, other)
        inner = jnp.zeros((1, ROWS), f32)
        for b in range(2):
            rows = pl.ds(b * 256, 256)
            part = (
                acc[rows]
                + jnp.dot(wg_v[other, rows], grads[0], preferred_element_type=f32)
                + jnp.dot(wu_v[other, rows], grads[1], preferred_element_type=f32)
            )
            scaled = gx[pl.ds(4 * b, 4), m].reshape(256, ROWS).astype(f32)
            inner = inner + jnp.sum(part * scaled, axis=0, keepdims=True)
            zs[m, pl.ds(4 * b, 4)] = part.astype(bf16).reshape(4, CHUNK, ROWS)
            if m == 0:
                acc[rows] = part
        for k in FAR_Z:
            to = at_col(k)
            remote(zs.at[m, to], zr.at[m, c], ss.at[6, m], rs.at[6, m], (s, r, to)).start()
        kzs[m] = inner
        for k in FAR_Z:
            remote(kzs.at[m], kzr.at[m, c], ss.at[8, m], rs.at[8, m], (s, r, at_col(k))).start()
        zr[m, c] = zs[m, c]
        kzr[m, c] = inner

    def early():
        known = carry[0] + inc_t[...] - cot_t[...]
        found = []
        for i in range(UPD):
            total = jnp.zeros((1, ROWS), f32)
            for b in range(2):
                scaled = gv[pl.ds(4 * b, 4), i].reshape(256, ROWS).astype(f32)
                total = total + jnp.sum(acc[pl.ds(b * 256, 256)] * scaled, axis=0, keepdims=True)
            found.append(rstd[0] * total + jnp.sum(v_t[i] * known, axis=0, keepdims=True))
        meet_row(jnp.concatenate([*found, kzs[0], jnp.zeros((7, ROWS), f32)], axis=0))

    def meet_row(part):
        dxs[...] = part
        dxr[r] = part
        for k in range(1, ROW):
            remote(dxs, dxr.at[r], one_s.at[5], one_r.at[5], (s, lax.rem(r + k, ROW), c)).start()

    def meet_col():
        arrived(dxr.at[pl.ds(0, ROW - 1)], one_r.at[5])
        part = jnp.sum(dxr[...], axis=0)
        dzs[...] = part
        dzr[c] = part
        for k in FAR_Z:
            remote(dzs, dzr.at[c], one_s.at[6], one_r.at[6], (s, r, at_col(k))).start()

    def updated(m):
        arrived(zr.at[m, pl.ds(0, COL - 1)], rs.at[6, m])
        arrived(kzr.at[m, pl.ds(0, COL - 1)], rs.at[8, m])
        total = jnp.sum(zr[m].astype(f32), axis=0)
        inner = jnp.sum(kzr[m], axis=0)
        root = rstd[m]
        fresh = carry[m] + root * (gain_t[...] * total)
        after[m] = fresh
        kps[m] = (root * root * root) * (inner / D)

        @pl.when(s != 0)
        def _():
            gys[m] = fresh.astype(bf16)
            for k in (*FAR_Z, 0):
                remote(
                    gys.at[m], gy.at[m, c], ss.at[0, m], rs.at[0, m], (s - 1, r, at_col(k))
                ).start()
            for k in range(ROW):
                remote(kps.at[m], kpr.at[m, r], ss.at[7, m], rs.at[7, m], (s - 1, lax.rem(r + k, ROW), c)).start()
            remote(after.at[m], carry.at[m], ss.at[1, m], rs.at[1, m], (s - 1, r, c)).start()

        @pl.when(s == 0)
        def _():
            if m == 0:
                home[...] = fresh
            else:
                remote(after.at[m], home, ss.at[1, m], one_r.at[4], (m, r, c)).start()
                for k in range(ROW):
                    remote(kps.at[m], khome.at[r], ss.at[7, m], one_r.at[10], (m, lax.rem(r + k, ROW), c)).start()

    def squares_met():
        total = jnp.sum(sqz[...], axis=0)
        sqm[...] = total
        sqx[r] = total
        for k in range(1, ROW):
            remote(sqm, sqx.at[r], one_s.at[3], one_r.at[3], (s, lax.rem(r + k, ROW), c)).start()

    def roots():
        arrived(sqx.at[pl.ds(0, ROW - 1)], one_r.at[3])
        root = lax.rsqrt(jnp.sum(sqx[...], axis=0) / D + eps)
        for m in range(MB):
            rstd[m] = root[m : m + 1]

    stages = {"V": halved, "S": summed, "P": spread, "F": features, "U": updated}

    def play(order, first):
        for step, m in order:
            if step == "H":
                hidden(m, first)
            elif step == "q":
                if first:
                    arrived(sqz.at[pl.ds(0, COL - 1)], one_r.at[2])
                squares_met()
            elif step == "r":
                roots()
            elif step == "g":
                arrived(gx.at[pl.ds(0, COL - 1)], one_r.at[1])
            elif step == "e":

                @pl.when(s == 0)
                def _():
                    early()

            elif step == "d":

                @pl.when(s == 0)
                def _():
                    meet_col()

            else:
                stages[step](m)
            if step == "V" and m and first:
                slopes(m - 1)

    @pl.when(s == LAST)
    def _():
        play(FIRST_ORDER, True)

    @pl.when(s != LAST)
    def _():
        play(ORDER, False)

    @pl.when(s == LAST)
    def _():
        leanings()
        leanings_met()

    @pl.when(s != 0)
    def _():
        arrived(home, one_r.at[4])
        rough = home[...] + inc_t[...] - cot_t[...]
        part = [jnp.sum(v_t[i] * rough, axis=0, keepdims=True) for i in range(UPD)]
        meet_row(jnp.concatenate([*part, jnp.zeros((8, ROWS), f32)], axis=0))
        meet_col()
        arrived(khome, one_r.at[10])
        kall[...] = jnp.sum(khome[...], axis=0)

    arrived(vzr.at[pl.ds(0, COL - 1)], one_r.at[12])
    arrived(dzr.at[pl.ds(0, COL - 1)], one_r.at[6])
    met = jnp.sum(dzr[...], axis=0)

    @pl.when(s == 0)
    def _():
        kall[...] = (rstd[0] * rstd[0] * rstd[0]) * (met[UPD : UPD + 1] / D)

    resid = home[...] - kall[...] * below[...].astype(f32) + inc_t[...] - cot_t[...]
    out_o[1] = resid
    dots = jnp.sum(met[:UPD] - kall[...] * jnp.sum(vzr[...], axis=0), axis=1, keepdims=True)
    update = dots[0:1] * u_t[0]
    for i in range(1, UPD):
        update = update + dots[i : i + 1] * u_t[i]
    out_o[0] = cot_t[...] + resid - update

    @pl.when(s == LAST)
    def _():
        left(gy.at[0, pl.ds(0, COL - 1)], first.at[0])

    @pl.when(s != LAST)
    def _():
        left(gy.at[0], first.at[0])
        left(cot_t, first.at[1])
        left(above_all.at[pl.ds(0, COL - 1)], one_s.at[9])

    @pl.when(s != 0)
    def _():
        left(x_v, one_s.at[7])

    @pl.when(s == 0)
    def _():
        left(gv.at[pl.ds(0, COL - 1)], one_s.at[13])
        left(x_v.at[pl.ds(1, MB - 1)], one_s.at[8])

    left(gx.at[pl.ds(0, COL - 1)], one_s.at[1])
    left(sqz.at[pl.ds(0, COL - 1)], one_s.at[2])
    left(sqx.at[pl.ds(0, ROW - 1)], one_s.at[3])
    left(vxr.at[pl.ds(0, ROW - 1)], one_s.at[11])
    left(vzr.at[pl.ds(0, COL - 1)], one_s.at[12])
    left(dxr.at[pl.ds(0, ROW - 1)], one_s.at[5])
    left(dzr.at[pl.ds(0, COL - 1)], one_s.at[6])

    def drained(m, carry_):
        @pl.when(s != 0)
        def _():
            left(gy.at[m], ss.at[0, m])

        @pl.when(jnp.logical_or(s != 0, m != 0))
        def _():
            left(after.at[m], ss.at[1, m])
            left(kpr.at[m], ss.at[7, m])

        left(d1s.at[m], ss.at[2, m])
        left(xrv.at[m, :, pl.ds(0, XS - 1)], ss.at[3, m])
        left(ga.at[m, core, pl.ds(0, XS - 1)], ss.at[4, m])
        left(ga.at[m, core], ss.at[5, m])
        left(zr.at[m, pl.ds(0, COL - 1)], ss.at[6, m])
        left(kzr.at[m, pl.ds(0, COL - 1)], ss.at[8, m])
        return carry_

    lax.fori_loop(0, MB, drained, 0)


def turned(a):
    return jnp.swapaxes(a, -1, -2)


def shards(cotangent, incoming, upd_u, upd_v, saved_x, saved_h, norm_gain, w_gate, w_up, w_down):
    vm = pltpu.VMEM
    dma = pltpu.SemaphoreType.DMA
    tile = (CHUNK, ROWS)
    out = pl.pallas_call(
        kernel,
        out_shape=jax.ShapeDtypeStruct((2, *tile), f32),
        in_specs=[pl.BlockSpec(memory_space=pl.ANY)] * 10,
        out_specs=pl.BlockSpec(memory_space=pltpu.VMEM),
        scratch_shapes=[
            vm(tile, f32),
            vm(tile, f32),
            vm((UPD, *tile), f32),
            vm((UPD, *tile), f32),
            vm((MB, *tile), bf16),
            vm((MB, 2, ROWS, HID), bf16),
            vm((1, CHUNK), f32),
            vm((2, FEATS, HALF), bf16),
            vm((2, FEATS, HALF), bf16),
            vm((ROW, PIECE, FEATS), bf16),
            vm((MB, *tile), f32),
            vm(tile, f32),
            vm((COL, MB, *tile), bf16),
            vm((COL, UPD, *tile), bf16),
            vm((MB, 2, 2, HALF, ROWS), f32),
            vm(tile, bf16),
            vm((MB, COL, *tile), bf16),
            vm((MB, *tile), bf16),
            vm((MB, *tile), f32),
            vm((MB, *tile), f32),
            vm((MB, PARTS, XS, PART, ROWS), bf16),
            vm((MB, PARTS, XS, PART, ROWS), bf16),
            vm((MB, PARTS, XS, PART, ROWS), f32),
            vm((MB, PARTS, XS, PART, ROWS), bf16),
            vm((MB, PARTS, XS, PART, ROWS), bf16),
            vm((MB, PARTS, PART, ROWS), f32),
            vm((MB, 2, XS, PARTS, PART, ROWS), bf16),
            vm((2, HALF, ROWS), bf16),
            vm((FEATS, ROWS), f32),
            vm((MB, COL, *tile), bf16),
            vm((MB, COL, *tile), bf16),
            vm((MB, 1, ROWS), f32),
            vm((MB, COL, 1, ROWS), f32),
            vm((MB, 1, ROWS), f32),
            vm((MB, ROW, 1, ROWS), f32),
            vm((MB, *tile), bf16),
            vm((COL, MB, *tile), bf16),
            vm((MB, ROW, PIECE, ROWS), f32),
            vm(tile, bf16),
            vm((8, ROWS), f32),
            vm((COL, 8, ROWS), f32),
            vm((8, ROWS), f32),
            vm((ROW, 8, ROWS), f32),
            vm((MB, 1, ROWS), f32),
            vm(tile, f32),
            vm((ROW, 1, ROWS), f32),
            vm((1, ROWS), f32),
            vm((UPD, ROWS), f32),
            vm((ROW, UPD, ROWS), f32),
            vm((UPD, ROWS), f32),
            vm((COL, UPD, ROWS), f32),
            vm((2 * UPD, ROWS), f32),
            vm((ROW, 2 * UPD, ROWS), f32),
            vm((2 * UPD, ROWS), f32),
            vm((COL, 2 * UPD, ROWS), f32),
            dma((12,)),
            dma((2,)),
            dma((9, MB)),
            dma((9, MB)),
            dma((2, PARTS, MB)),
            dma((14,)),
            dma((14,)),
        ],
        compiler_params=pltpu.CompilerParams(
            collective_id=0, has_side_effects=True, vmem_limit_bytes=60 * 1024 * 1024
        ),
        name="broyden",
    )(
        turned(cotangent), turned(incoming), turned(upd_u), turned(upd_v), turned(saved_x), saved_h, norm_gain,
        w_gate, w_up, w_down.reshape(1, ROW, PIECE, FEATS),
    )
    return out[0].T[None], out[1].T[None]


def solution(mesh):
    placed = (
        P("section", None, ("row", "col")),
        P("section", None, ("row", "col")),
        P("section", None, None, ("row", "col")),
        P("section", None, None, ("row", "col")),
        P("section", None, None, ("row", "col")),
        P("section", None, None, None, "col"),
        P("section", ("row", "col")),
        P("section", "row", "col"),
        P("section", "row", "col"),
        P("section", "col", "row"),
    )
    return jax.shard_map(
        shards,
        mesh=mesh,
        in_specs=placed,
        out_specs=(P("section", None, ("row", "col")), P("section", None, ("row", "col"))),
        check_vma=False,
    )
```

```python
import jax
import jax.numpy as jnp
from jax import lax
from jax.experimental import pallas as pl
from jax.experimental.pallas import tpu as pltpu
from jax.sharding import PartitionSpec as P

D = 4096
FF = 14336
ROWS = 128
UPD = 8
MB = 4
SECTIONS, ROW, COL = 4, 8, 8
XS = ROW // 2
CHUNK = D // (ROW * COL)
FEATS = D // ROW
HID = FF // COL
HALF = HID // 2
PIECE = HID // ROW
PARTS = 2
PART = PIECE // PARTS
STRIP = CHUNK // PARTS
FAR_Z = (4, 3, 5, 2, 6, 1, 7)
FAR_X = (2, 1, 3)
FIRST_ORDER = [
    ("H", 3), ("V", 3), ("S", 3), ("H", 2), ("V", 2), ("q", 0), ("P", 3), ("g", 0), ("F", 3), ("S", 2),
    ("H", 1), ("V", 1), ("r", 0), ("U", 3), ("P", 2), ("F", 2), ("S", 1), ("H", 0), ("V", 0), ("U", 2),
    ("P", 1), ("F", 1), ("S", 0), ("U", 1), ("P", 0), ("F", 0), ("U", 0),
]
ORDER = [
    ("H", 3), ("V", 3), ("S", 3), ("H", 2), ("V", 2), ("q", 0), ("P", 3), ("g", 0), ("F", 3), ("S", 2),
    ("H", 1), ("V", 1), ("r", 0), ("U", 3), ("P", 2), ("F", 2), ("S", 1), ("H", 0), ("V", 0), ("U", 2),
    ("P", 1), ("F", 1), ("S", 0), ("U", 1), ("P", 0), ("F", 0), ("e", 0), ("d", 0), ("U", 0),
]

eps = 1e-05
bf16 = jnp.bfloat16
f32 = jnp.float32
MESH = pl.DeviceIdType.MESH


def kernel(
    cot_h, inc_h, u_h, v_h, x_h, h_h, gain_h, wg_h, wu_h, wd_h,
    out_o,
    cot_t, inc_t, u_t, v_t, x_v, h_v, gain_v, wg_v, wu_v, wd_v,
    x_t, gain_t, gx, gv, slope,
    start, gy, gys, carry, after, d1s, d1r, own, xsd, xrv, mine, ga, grads, acc, zs, zr,
    kzs, kzr, kps, kpr, above, above_all, lean, below, sqs, sqz, sqm, sqx, rstd, home, khome, kall, vxs, vxr, vzs, vzr, dxs, dxr, dzs, dzr,
    load, first, ss, rs, split, one_s, one_r,
):
    s = lax.axis_index("section")
    r = lax.axis_index("row")
    c = lax.axis_index("col")
    core = lax.rem(r, 2)
    x = lax.div(r, 2)
    mate = r + 1 - 2 * core

    def at_col(k):
        return lax.rem(c + k, COL)

    def at_x(k):
        return lax.rem(x + k, XS)

    def remote(src, dst, send, recv, device):
        return pltpu.make_async_remote_copy(
            src_ref=src, dst_ref=dst, send_sem=send, recv_sem=recv, device_id=device, device_id_type=MESH
        )

    def arrived(ref, recv):
        remote(ref, ref, one_s.at[0], recv, (s, mate, c)).wait_recv()

    def left(ref, send):
        remote(ref, ref, send, one_r.at[0], (s, mate, c)).wait_send()

    barrier = pltpu.get_barrier_semaphore()
    for k in FAR_Z:
        pl.semaphore_signal(barrier, inc=1, device_id=(s, r, at_col(k)), device_id_type=MESH)
    for k in (2, 1, 3):
        pl.semaphore_signal(barrier, inc=1, device_id=(lax.rem(s + k, SECTIONS), r, c), device_id_type=MESH)
    for k in range(1, ROW):
        pl.semaphore_signal(barrier, inc=1, device_id=(s, lax.rem(r + k, ROW), c), device_id_type=MESH)

    loads = {}
    for i, (name, src, dst) in enumerate(
        (
            ("cot", cot_h.at[0], cot_t),
            ("gain", gain_h, gain_v),
            ("x", x_h.at[0], x_v),
            ("wd", wd_h.at[0], wd_v),
            ("h", h_h.at[0], h_v),
            ("wg0", wg_h.at[0, :, pl.ds(0, HALF)], wg_v.at[0]),
            ("wg1", wg_h.at[0, :, pl.ds(HALF, HALF)], wg_v.at[1]),
            ("wu0", wu_h.at[0, :, pl.ds(0, HALF)], wu_v.at[0]),
            ("wu1", wu_h.at[0, :, pl.ds(HALF, HALF)], wu_v.at[1]),
            ("inc", inc_h.at[0], inc_t),
            ("u", u_h.at[0], u_t),
            ("v", v_h.at[0], v_t),
        )
    ):
        loads[name] = pltpu.make_async_copy(src, dst, load.at[i])
        loads[name].start()

    loads["cot"].wait()
    start[...] = cot_t[...].astype(bf16)
    pl.semaphore_wait(barrier, SECTIONS - 1 + COL - 1 + ROW - 1)

    LAST = SECTIONS - 1
    mb_home = s

    @pl.when(s == LAST)
    def _():
        gy[LAST, c] = start[...]
        carry[LAST] = cot_t[...]
        for k in FAR_Z:
            remote(
                start, gy.at[LAST, c], first.at[0], rs.at[0, LAST], (LAST, r, at_col(k))
            ).start()

    loads["x"].wait()

    @pl.when(s != 0)
    def _():
        remote(x_v, above, one_s.at[7], one_r.at[7], (s - 1, r, c)).start()

    @pl.when(s == 0)
    def _():
        for m in range(1, MB):
            remote(x_v.at[m], below, one_s.at[8], one_r.at[8], (m, r, c)).start()
        below[...] = x_v[0]

    loads["gain"].wait()
    gain_t[...] = jnp.broadcast_to(gain_v[...], (ROWS, CHUNK)).T
    sums = []
    for m in range(MB):
        xt = x_v[m].astype(f32)
        x_t[m] = xt
        gx[c, m] = (gain_t[...] * xt).astype(bf16)
        sums.append(jnp.sum(xt * xt, axis=0, keepdims=True))
    sums = jnp.concatenate(sums + sums, axis=0)
    sqs[...] = sums
    sqz[c] = sums
    for k in FAR_Z:
        remote(sqs, sqz.at[c], one_s.at[2], one_r.at[2], (s, r, at_col(k))).start()

    @pl.when(s != LAST)
    def _():
        arrived(sqz.at[pl.ds(0, COL - 1)], one_r.at[2])
        for k in (*FAR_Z, 0):
            remote(start, gy.at[mb_home, c], first.at[0], rs.at[0, mb_home], (LAST, r, at_col(k))).start()
        remote(cot_t, carry.at[mb_home], first.at[1], rs.at[1, mb_home], (LAST, r, c)).start()
        arrived(above, one_r.at[7])
        above_all[c] = above[...]
        for k in FAR_Z:
            remote(above, above_all.at[c], one_s.at[9], one_r.at[9], (s, r, at_col(k))).start()

    for k in FAR_Z:
        remote(gx.at[c], gx.at[c], one_s.at[1], one_r.at[1], (s, r, at_col(k))).start()

    def slopes(m):
        for half in range(2):
            for b in range(7):
                at = pl.ds(half * HALF + b * 128, 128)
                hg = h_v[m, 0, :, at].astype(f32)
                hu = h_v[m, 1, :, at].astype(f32)
                sig = jax.nn.sigmoid(hg)
                slope[m, 0, half, pl.ds(b * 128, 128)] = (hu * sig * (1.0 + hg * (1.0 - sig))).T
                slope[m, 1, half, pl.ds(b * 128, 128)] = (hg * sig).T

    loads["h"].wait()
    loads["inc"].wait()
    loads["u"].wait()
    loads["v"].wait()

    @pl.when(s != LAST)
    def _():
        def body(m, carry_):
            slopes(m)
            return carry_

        lax.fori_loop(0, MB, body, 0)

    @pl.when(s == LAST)
    def _():
        slopes(LAST)

    for name in ("wd", "wg0", "wg1", "wu0", "wu1"):
        loads[name].wait()

    def leanings():
        @pl.when(s != 0)
        def _():
            arrived(below, one_r.at[8])

        b = below[...].astype(f32)
        part = jnp.concatenate([jnp.sum(v_t[i] * b, axis=0, keepdims=True) for i in range(UPD)], axis=0)
        vxs[...] = part
        vxr[r] = part
        for k in range(1, ROW):
            remote(vxs, vxr.at[r], one_s.at[11], one_r.at[11], (s, lax.rem(r + k, ROW), c)).start()

    def leanings_met():
        arrived(vxr.at[pl.ds(0, ROW - 1)], one_r.at[11])
        part = jnp.sum(vxr[...], axis=0)
        vzs[...] = part
        vzr[c] = part
        for k in FAR_Z:
            remote(vzs, vzr.at[c], one_s.at[12], one_r.at[12], (s, r, at_col(k))).start()

    @pl.when(s != LAST)
    def _():
        leanings()

    @pl.when(s == 0)
    def _():
        for i in range(UPD):
            gv[c, i] = (gain_t[...] * v_t[i]).astype(bf16)
        for k in FAR_Z:
            remote(gv.at[c], gv.at[c], one_s.at[13], one_r.at[13], (s, r, at_col(k))).start()

    @pl.when(s != LAST)
    def _():
        arrived(above_all.at[pl.ds(0, COL - 1)], one_r.at[9])

        def body(m, carry_):
            a = above_all[:, m].reshape(FEATS, ROWS)
            for i in range(ROW):
                lean[m, i] = jnp.dot(wd_v[i], a, preferred_element_type=f32)
            return carry_

        lax.fori_loop(0, MB, body, 0)
        leanings_met()

    @pl.when(s == 0)
    def _():
        arrived(gv.at[pl.ds(0, COL - 1)], one_r.at[13])

    def hidden(m, first):
        if first and m == LAST:
            arrived(gy.at[m, pl.ds(0, COL - 1)], rs.at[0, m])
        else:
            arrived(gy.at[m], rs.at[0, m])
            arrived(carry.at[m], rs.at[1, m])
        if not first:
            arrived(kpr.at[m], rs.at[7, m])
            k = jnp.sum(kpr[m], axis=0)
        g = gy[m].reshape(FEATS, ROWS)

        def product(q, b):
            rows = pl.ds(b * PART, PART)
            whole = jnp.dot(wd_v[q, rows], g, preferred_element_type=f32)
            return whole if first else whole - k * lean[m, q, rows]

        for b in range(PARTS):
            for i in range(XS):
                d1s[m, b, i] = product((1 - core) * XS + i, b).astype(bf16)
            remote(d1s.at[m, b], d1r.at[m, b], ss.at[2, m], split.at[0, b, m], (s, mate, c)).start()
        for b in range(PARTS):
            for i in range(XS):
                own[m, b, i] = product(core * XS + i, b)
        if not first:
            carry[m] = carry[m] - k * above[m].astype(f32)

    def halved(m):
        for b in range(PARTS):
            arrived(d1r.at[m, b], split.at[0, b, m])
            for k in FAR_X:
                to = at_x(k)
                xsd[m, b, to] = (own[m, b, to] + d1r[m, b, to].astype(f32)).astype(bf16)
                remote(
                    xsd.at[m, b, to], xrv.at[m, b, x], ss.at[3, m], split.at[1, b, m], (s, 2 * to + core, c)
                ).start()
            mine[m, b] = own[m, b, x] + d1r[m, b, x].astype(f32)

    def summed(m):
        for b in range(PARTS):
            arrived(xrv.at[m, b, pl.ds(0, XS - 1)], split.at[1, b, m])
            total = mine[m, b]
            for k in FAR_X:
                total = total + xrv[m, b, at_x(k)].astype(f32)
            ga[m, core, x, b] = total.astype(bf16)
            for k in FAR_X:
                remote(
                    ga.at[m, core, x, b], ga.at[m, core, x, b], ss.at[4, m], rs.at[4, m], (s, 2 * at_x(k) + core, c)
                ).start()

    def gradients(m, half):
        g = ga[m, half].reshape(HALF, ROWS).astype(f32)
        grads[0] = (g * slope[m, 0, half]).astype(bf16)
        grads[1] = (g * slope[m, 1, half]).astype(bf16)

    def spread(m):
        arrived(ga.at[m, core, pl.ds(0, XS - 1)], rs.at[4, m])
        remote(ga.at[m, core], ga.at[m, core], ss.at[5, m], rs.at[5, m], (s, mate, c)).start()
        gradients(m, core)
        for b in range(2):
            rows = pl.ds(b * 256, 256)
            acc[rows] = jnp.dot(wg_v[core, rows], grads[0], preferred_element_type=f32) + jnp.dot(
                wu_v[core, rows], grads[1], preferred_element_type=f32
            )

    def features(m):
        other = 1 - core
        arrived(ga.at[m, other], rs.at[5, m])
        gradients(m, other)
        inner = jnp.zeros((1, ROWS), f32)
        for b in range(2):
            rows = pl.ds(b * 256, 256)
            part = (
                acc[rows]
                + jnp.dot(wg_v[other, rows], grads[0], preferred_element_type=f32)
                + jnp.dot(wu_v[other, rows], grads[1], preferred_element_type=f32)
            )
            scaled = gx[pl.ds(4 * b, 4), m].reshape(256, ROWS).astype(f32)
            inner = inner + jnp.sum(part * scaled, axis=0, keepdims=True)
            zs[m, pl.ds(4 * b, 4)] = part.astype(bf16).reshape(4, CHUNK, ROWS)
            if m == 0:
                acc[rows] = part
        for b in range(PARTS):
            rows = pl.ds(b * STRIP, STRIP)
            for k in FAR_Z:
                to = at_col(k)
                remote(
                    zs.at[m, to, rows], zr.at[m, c, rows], ss.at[6, m], split.at[2, b, m], (s, r, to)
                ).start()
        kzs[m] = inner
        for k in FAR_Z:
            remote(kzs.at[m], kzr.at[m, c], ss.at[8, m], rs.at[8, m], (s, r, at_col(k))).start()
        zr[m, c] = zs[m, c]
        kzr[m, c] = inner

    def early():
        known = carry[0] + inc_t[...] - cot_t[...]
        found = []
        for i in range(UPD):
            total = jnp.zeros((1, ROWS), f32)
            for b in range(2):
                scaled = gv[pl.ds(4 * b, 4), i].reshape(256, ROWS).astype(f32)
                total = total + jnp.sum(acc[pl.ds(b * 256, 256)] * scaled, axis=0, keepdims=True)
            found.append(rstd[0] * total + jnp.sum(v_t[i] * known, axis=0, keepdims=True))
        meet_row(jnp.concatenate([*found, kzs[0], jnp.zeros((7, ROWS), f32)], axis=0))

    def meet_row(part):
        dxs[...] = part
        dxr[r] = part
        for k in range(1, ROW):
            remote(dxs, dxr.at[r], one_s.at[5], one_r.at[5], (s, lax.rem(r + k, ROW), c)).start()

    def meet_col():
        arrived(dxr.at[pl.ds(0, ROW - 1)], one_r.at[5])
        part = jnp.sum(dxr[...], axis=0)
        dzs[...] = part
        dzr[c] = part
        for k in FAR_Z:
            remote(dzs, dzr.at[c], one_s.at[6], one_r.at[6], (s, r, at_col(k))).start()

    def updated(m):
        root = rstd[m]
        for b in range(PARTS):
            rows = pl.ds(b * STRIP, STRIP)
            arrived(zr.at[m, pl.ds(0, COL - 1), rows], split.at[2, b, m])
            total = jnp.sum(zr[m, :, rows].astype(f32), axis=0)
            fresh = carry[m, rows] + root * (gain_t[rows] * total)
            after[m, rows] = fresh

            @pl.when(s != 0)
            def _():
                gys[m, rows] = fresh.astype(bf16)
                for k in (*FAR_Z, 0):
                    remote(
                        gys.at[m, rows], gy.at[m, c, rows], ss.at[0, m], rs.at[0, m], (s - 1, r, at_col(k))
                    ).start()

        arrived(kzr.at[m, pl.ds(0, COL - 1)], rs.at[8, m])
        kps[m] = (root * root * root) * (jnp.sum(kzr[m], axis=0) / D)

        @pl.when(s != 0)
        def _():
            for k in range(ROW):
                remote(kps.at[m], kpr.at[m, r], ss.at[7, m], rs.at[7, m], (s - 1, lax.rem(r + k, ROW), c)).start()
            remote(after.at[m], carry.at[m], ss.at[1, m], rs.at[1, m], (s - 1, r, c)).start()

        @pl.when(s == 0)
        def _():
            if m == 0:
                home[...] = after[m]
            else:
                remote(after.at[m], home, ss.at[1, m], one_r.at[4], (m, r, c)).start()
                for k in range(ROW):
                    remote(kps.at[m], khome.at[r], ss.at[7, m], one_r.at[10], (m, lax.rem(r + k, ROW), c)).start()

    def squares_met():
        total = jnp.sum(sqz[...], axis=0)
        sqm[...] = total
        sqx[r] = total
        for k in range(1, ROW):
            remote(sqm, sqx.at[r], one_s.at[3], one_r.at[3], (s, lax.rem(r + k, ROW), c)).start()

    def roots():
        arrived(sqx.at[pl.ds(0, ROW - 1)], one_r.at[3])
        root = lax.rsqrt(jnp.sum(sqx[...], axis=0) / D + eps)
        for m in range(MB):
            rstd[m] = root[m : m + 1]

    stages = {"V": halved, "S": summed, "P": spread, "F": features, "U": updated}

    def play(order, first):
        for step, m in order:
            if step == "H":
                hidden(m, first)
            elif step == "q":
                if first:
                    arrived(sqz.at[pl.ds(0, COL - 1)], one_r.at[2])
                squares_met()
            elif step == "r":
                roots()
            elif step == "g":
                arrived(gx.at[pl.ds(0, COL - 1)], one_r.at[1])
            elif step == "e":

                @pl.when(s == 0)
                def _():
                    early()

            elif step == "d":

                @pl.when(s == 0)
                def _():
                    meet_col()

            else:
                stages[step](m)
            if step == "V" and m and first:
                slopes(m - 1)

    @pl.when(s == LAST)
    def _():
        play(FIRST_ORDER, True)

    @pl.when(s != LAST)
    def _():
        play(ORDER, False)

    @pl.when(s == LAST)
    def _():
        leanings()
        leanings_met()

    @pl.when(s != 0)
    def _():
        arrived(home, one_r.at[4])
        rough = home[...] + inc_t[...] - cot_t[...]
        part = [jnp.sum(v_t[i] * rough, axis=0, keepdims=True) for i in range(UPD)]
        meet_row(jnp.concatenate([*part, jnp.zeros((8, ROWS), f32)], axis=0))
        meet_col()
        arrived(khome, one_r.at[10])
        kall[...] = jnp.sum(khome[...], axis=0)

    arrived(vzr.at[pl.ds(0, COL - 1)], one_r.at[12])
    arrived(dzr.at[pl.ds(0, COL - 1)], one_r.at[6])
    met = jnp.sum(dzr[...], axis=0)

    @pl.when(s == 0)
    def _():
        kall[...] = (rstd[0] * rstd[0] * rstd[0]) * (met[UPD : UPD + 1] / D)

    resid = home[...] - kall[...] * below[...].astype(f32) + inc_t[...] - cot_t[...]
    out_o[1] = resid
    dots = jnp.sum(met[:UPD] - kall[...] * jnp.sum(vzr[...], axis=0), axis=1, keepdims=True)
    update = dots[0:1] * u_t[0]
    for i in range(1, UPD):
        update = update + dots[i : i + 1] * u_t[i]
    out_o[0] = cot_t[...] + resid - update

    @pl.when(s == LAST)
    def _():
        left(gy.at[0, pl.ds(0, COL - 1)], first.at[0])

    @pl.when(s != LAST)
    def _():
        left(gy.at[0], first.at[0])
        left(cot_t, first.at[1])
        left(above_all.at[pl.ds(0, COL - 1)], one_s.at[9])

    @pl.when(s != 0)
    def _():
        left(x_v, one_s.at[7])

    @pl.when(s == 0)
    def _():
        left(gv.at[pl.ds(0, COL - 1)], one_s.at[13])
        left(x_v.at[pl.ds(1, MB - 1)], one_s.at[8])

    left(gx.at[pl.ds(0, COL - 1)], one_s.at[1])
    left(sqz.at[pl.ds(0, COL - 1)], one_s.at[2])
    left(sqx.at[pl.ds(0, ROW - 1)], one_s.at[3])
    left(vxr.at[pl.ds(0, ROW - 1)], one_s.at[11])
    left(vzr.at[pl.ds(0, COL - 1)], one_s.at[12])
    left(dxr.at[pl.ds(0, ROW - 1)], one_s.at[5])
    left(dzr.at[pl.ds(0, COL - 1)], one_s.at[6])

    def drained(m, carry_):
        @pl.when(s != 0)
        def _():
            left(gy.at[m], ss.at[0, m])

        @pl.when(jnp.logical_or(s != 0, m != 0))
        def _():
            left(after.at[m], ss.at[1, m])
            left(kpr.at[m], ss.at[7, m])

        left(d1s.at[m], ss.at[2, m])
        left(xrv.at[m, :, pl.ds(0, XS - 1)], ss.at[3, m])
        left(ga.at[m, core, pl.ds(0, XS - 1)], ss.at[4, m])
        left(ga.at[m, core], ss.at[5, m])
        left(zr.at[m, pl.ds(0, COL - 1)], ss.at[6, m])
        left(kzr.at[m, pl.ds(0, COL - 1)], ss.at[8, m])
        return carry_

    lax.fori_loop(0, MB, drained, 0)


def turned(a):
    return jnp.swapaxes(a, -1, -2)


def shards(cotangent, incoming, upd_u, upd_v, saved_x, saved_h, norm_gain, w_gate, w_up, w_down):
    vm = pltpu.VMEM
    dma = pltpu.SemaphoreType.DMA
    tile = (CHUNK, ROWS)
    out = pl.pallas_call(
        kernel,
        out_shape=jax.ShapeDtypeStruct((2, *tile), f32),
        in_specs=[pl.BlockSpec(memory_space=pl.ANY)] * 10,
        out_specs=pl.BlockSpec(memory_space=pltpu.VMEM),
        scratch_shapes=[
            vm(tile, f32),
            vm(tile, f32),
            vm((UPD, *tile), f32),
            vm((UPD, *tile), f32),
            vm((MB, *tile), bf16),
            vm((MB, 2, ROWS, HID), bf16),
            vm((1, CHUNK), f32),
            vm((2, FEATS, HALF), bf16),
            vm((2, FEATS, HALF), bf16),
            vm((ROW, PIECE, FEATS), bf16),
            vm((MB, *tile), f32),
            vm(tile, f32),
            vm((COL, MB, *tile), bf16),
            vm((COL, UPD, *tile), bf16),
            vm((MB, 2, 2, HALF, ROWS), f32),
            vm(tile, bf16),
            vm((MB, COL, *tile), bf16),
            vm((MB, *tile), bf16),
            vm((MB, *tile), f32),
            vm((MB, *tile), f32),
            vm((MB, PARTS, XS, PART, ROWS), bf16),
            vm((MB, PARTS, XS, PART, ROWS), bf16),
            vm((MB, PARTS, XS, PART, ROWS), f32),
            vm((MB, PARTS, XS, PART, ROWS), bf16),
            vm((MB, PARTS, XS, PART, ROWS), bf16),
            vm((MB, PARTS, PART, ROWS), f32),
            vm((MB, 2, XS, PARTS, PART, ROWS), bf16),
            vm((2, HALF, ROWS), bf16),
            vm((FEATS, ROWS), f32),
            vm((MB, COL, *tile), bf16),
            vm((MB, COL, *tile), bf16),
            vm((MB, 1, ROWS), f32),
            vm((MB, COL, 1, ROWS), f32),
            vm((MB, 1, ROWS), f32),
            vm((MB, ROW, 1, ROWS), f32),
            vm((MB, *tile), bf16),
            vm((COL, MB, *tile), bf16),
            vm((MB, ROW, PIECE, ROWS), f32),
            vm(tile, bf16),
            vm((8, ROWS), f32),
            vm((COL, 8, ROWS), f32),
            vm((8, ROWS), f32),
            vm((ROW, 8, ROWS), f32),
            vm((MB, 1, ROWS), f32),
            vm(tile, f32),
            vm((ROW, 1, ROWS), f32),
            vm((1, ROWS), f32),
            vm((UPD, ROWS), f32),
            vm((ROW, UPD, ROWS), f32),
            vm((UPD, ROWS), f32),
            vm((COL, UPD, ROWS), f32),
            vm((2 * UPD, ROWS), f32),
            vm((ROW, 2 * UPD, ROWS), f32),
            vm((2 * UPD, ROWS), f32),
            vm((COL, 2 * UPD, ROWS), f32),
            dma((12,)),
            dma((2,)),
            dma((9, MB)),
            dma((9, MB)),
            dma((3, PARTS, MB)),
            dma((14,)),
            dma((14,)),
        ],
        compiler_params=pltpu.CompilerParams(
            collective_id=0, has_side_effects=True, vmem_limit_bytes=60 * 1024 * 1024
        ),
        name="broyden",
    )(
        turned(cotangent), turned(incoming), turned(upd_u), turned(upd_v), turned(saved_x), saved_h, norm_gain,
        w_gate, w_up, w_down.reshape(1, ROW, PIECE, FEATS),
    )
    return out[0].T[None], out[1].T[None]


def solution(mesh):
    placed = (
        P("section", None, ("row", "col")),
        P("section", None, ("row", "col")),
        P("section", None, None, ("row", "col")),
        P("section", None, None, ("row", "col")),
        P("section", None, None, ("row", "col")),
        P("section", None, None, None, "col"),
        P("section", ("row", "col")),
        P("section", "row", "col"),
        P("section", "row", "col"),
        P("section", "col", "row"),
    )
    return jax.shard_map(
        shards,
        mesh=mesh,
        in_specs=placed,
        out_specs=(P("section", None, ("row", "col")), P("section", None, ("row", "col"))),
        check_vma=False,
    )
```
